8 devices in a mesh: parts: 1 (over z), tiley: 2 (over y), tilex: 4 (over x, core).
Axes of the slice: x: 2, y: 2, z: 1, core: 2. Of those that a mesh axis runs over, the one named last changes fastest.
Arguments:
- node_feats: bfloat16 [16384, 1433], P(('parts', 'tiley', 'tilex'))
- adj_int: bfloat16 [16384, 2048], P(('parts', 'tiley', 'tilex'))
- adj_halo: bfloat16 [16384, 1024], P(('parts', 'tiley', 'tilex'))
- send_idx: int32 [32, 256], P(('parts', 'tiley', 'tilex'))
- w_hidden: bfloat16 [1433, 16], replicated
- w_out: bfloat16 [16, 7], replicated
Outputs:
- output: bfloat16 [16384, 7], P(('parts', 'tiley', 'tilex'))
All inputs are finite; a program needn't handle non-finite values.
Results may differ from the reference program's by a relative error of at most 0.001.
Values are sent between devices in bfloat16 or wider.
A program may use at most 1 GiB of HBM per device.

```python
import jax
import jax.numpy as jnp
from jax import lax

GRID_Y = 2
GRID_X = 4
NODES_DEV = 2048
HALO_ROWS = 256
FEAT_IN = 1433
HIDDEN = 16
CLASSES = 7
TILES = GRID_Y * GRID_X


def tile_blocks(tile_key, recv_count, w_low, w_high):
    key_int, key_wint, key_halo, key_whalo = jax.random.split(tile_key, 4)
    row_ids = jnp.arange(NODES_DEV)[:, None]
    col_ids = jnp.arange(NODES_DEV)[None, :]
    int_mask = (jax.random.randint(key_int, (NODES_DEV, NODES_DEV), 0, NODES_DEV) < 16) | (row_ids == col_ids)
    int_w = jnp.where(int_mask, jax.random.uniform(key_wint, (NODES_DEV, NODES_DEV), jnp.float32, w_low, w_high), 0.0)
    slot_ids = jnp.arange(4 * HALO_ROWS)
    block_ids = slot_ids // HALO_ROWS
    region_lo = (2 * HALO_ROWS * (block_ids ^ 1))[None, :]
    in_region = (row_ids >= region_lo) & (row_ids < region_lo + 2 * HALO_ROWS)
    used_slot = (slot_ids % HALO_ROWS) < recv_count[block_ids]
    halo_mask = (jax.random.randint(key_halo, (NODES_DEV, 4 * HALO_ROWS), 0, HALO_ROWS) < 16) & in_region & used_slot[None, :]
    halo_w = jnp.where(halo_mask, jax.random.uniform(key_whalo, (NODES_DEV, 4 * HALO_ROWS), jnp.float32, w_low, w_high), 0.0)
    row_scale = lax.rsqrt(jnp.sum(int_w * int_w, axis=1, keepdims=True) + jnp.sum(halo_w * halo_w, axis=1, keepdims=True))
    return (int_w * row_scale).astype(jnp.bfloat16), (halo_w * row_scale).astype(jnp.bfloat16)


def draw_graph(graph_key, w_low, w_high):
    key_cnt, key_perm, key_tile = jax.random.split(graph_key, 3)
    counts = jax.random.randint(key_cnt, (TILES, 4), HALO_ROWS // 4, HALO_ROWS + 1)
    counts = counts.at[0, 0].set(HALO_ROWS)
    picked = jax.vmap(lambda pick_num: jax.random.permutation(jax.random.fold_in(key_perm, pick_num), 2 * HALO_ROWS)[:HALO_ROWS])(jnp.arange(TILES * 4))
    picked = picked.reshape(TILES, 4, HALO_ROWS) + (2 * HALO_ROWS * jnp.arange(4))[None, :, None]
    slot_ids = jnp.arange(HALO_ROWS)[None, None, :]
    send_idx = jnp.where(slot_ids < counts[:, :, None], picked, 0).astype(jnp.int32).reshape(TILES * 4, HALO_ROWS)
    grid_cnt = counts.reshape(GRID_Y, GRID_X, 4)
    recv_cnt = jnp.stack([
        jnp.roll(grid_cnt[:, :, 0], 1, axis=1),
        jnp.roll(grid_cnt[:, :, 1], -1, axis=1),
        jnp.roll(grid_cnt[:, :, 2], 1, axis=0),
        jnp.roll(grid_cnt[:, :, 3], -1, axis=0)], axis=-1).reshape(TILES, 4)
    adj_int, adj_halo = lax.map(lambda tile_num: tile_blocks(jax.random.fold_in(key_tile, tile_num), recv_cnt[tile_num], w_low, w_high), jnp.arange(TILES))
    return adj_int.reshape(TILES * NODES_DEV, NODES_DEV), adj_halo.reshape(TILES * NODES_DEV, 4 * HALO_ROWS), send_idx


def setup_inputs(seed: int = 0, part: int = 0) -> dict:
    part_key = jax.random.fold_in(jax.random.key(seed), part)
    key_graph, key_feat = jax.random.split(part_key, 2)
    key_first, key_second = jax.random.split(jax.random.key(seed + 1), 2)
    adj_int, adj_halo, send_idx = draw_graph(key_graph, 0.5, 1.5)
    node_feats = jax.random.normal(key_feat, (TILES * NODES_DEV, FEAT_IN), jnp.float32).astype(jnp.bfloat16)
    w_hidden = (jax.random.normal(key_first, (FEAT_IN, HIDDEN), jnp.float32) * FEAT_IN ** -0.5).astype(jnp.bfloat16)
    w_out = (jax.random.normal(key_second, (HIDDEN, CLASSES), jnp.float32) * HIDDEN ** -0.5).astype(jnp.bfloat16)
    return {'node_feats': node_feats, 'adj_int': adj_int, 'adj_halo': adj_halo, 'send_idx': send_idx, 'w_hidden': w_hidden, 'w_out': w_out}


def aggregate(layer_in, adj_int, adj_halo, send_idx):
    feat_width = layer_in.shape[1]
    own_rows = layer_in.reshape(TILES, NODES_DEV, feat_width)
    send_plans = send_idx.reshape(TILES, 4 * HALO_ROWS)
    sent_rows = jax.vmap(lambda tile_rows, tile_plan: tile_rows[tile_plan])(own_rows, send_plans)
    sent_rows = sent_rows.reshape(GRID_Y, GRID_X, 4, HALO_ROWS, feat_width)
    recv_rows = jnp.stack([
        jnp.roll(sent_rows[:, :, 0], 1, axis=1),
        jnp.roll(sent_rows[:, :, 1], -1, axis=1),
        jnp.roll(sent_rows[:, :, 2], 1, axis=0),
        jnp.roll(sent_rows[:, :, 3], -1, axis=0)], axis=2).reshape(TILES, 4 * HALO_ROWS, feat_width)

    def one_tile(tile_args):
        int_block, halo_block, tile_rows, tile_recv = tile_args
        agg_sum = jnp.dot(int_block, tile_rows, preferred_element_type=jnp.float32) + jnp.dot(halo_block, tile_recv, preferred_element_type=jnp.float32)
        return agg_sum.astype(jnp.bfloat16)

    agg_out = lax.map(one_tile, (adj_int.reshape(TILES, NODES_DEV, NODES_DEV), adj_halo.reshape(TILES, NODES_DEV, 4 * HALO_ROWS), own_rows, recv_rows))
    return agg_out.reshape(TILES * NODES_DEV, feat_width)


def reference(node_feats, adj_int, adj_halo, send_idx, w_hidden, w_out):
    z_first = aggregate(node_feats, adj_int, adj_halo, send_idx)
    hidden = jax.nn.relu(jnp.dot(z_first, w_hidden, preferred_element_type=jnp.float32)).astype(jnp.bfloat16)
    z_second = aggregate(hidden, adj_int, adj_halo, send_idx)
    return jnp.dot(z_second, w_out, preferred_element_type=jnp.float32).astype(jnp.bfloat16)
```

```python
import functools

import jax
import jax.numpy as jnp
from jax import lax
from jax.experimental import pallas as pl
from jax.experimental.pallas import tpu as pltpu
from jax.sharding import PartitionSpec as P

BF16 = jnp.bfloat16
F32 = jnp.float32
MESH = pl.DeviceIdType.MESH
N_TILE = 256
NN = (((1,), (0,)), ((), ()))
NT = (((1,), (1,)), ((), ()))


def dot(lhs, rhs, dims):
    return lax.dot_general(lhs, rhs, dims, preferred_element_type=F32)


def feature_chunks(feat):
    cuts = [0, 128]
    while feat - cuts[-1] > 512:
        cuts.append(cuts[-1] + 256)
    if feat - cuts[-1] > 256:
        cuts.append(cuts[-1] + 128)
    cuts.append(feat)
    return list(zip(cuts[:-1], cuts[1:]))


def gcn_kernel(grid_y, grid_x, chunks, idx_ref, w0_ref, w1_ref, feat_hbm, int_hbm, halo_hbm, out_ref,
               feat_v, int_v, halo_v, pick_v, send_y, send_x0, send_x1, recv_y, recv_x, z_int, hid_acc,
               hid_v, send2_y, send2_x0, send2_x1, recv2_y, recv2_x,
               feat_sem, int_sem, halo_sem, sy_sem, ry_sem, sx_sem, rx_sem, s2_sem, r2_sem):
    me_y = lax.axis_index('tiley')
    me_x = lax.axis_index('tilex')
    east = {'tilex': lax.rem(me_x + 1, grid_x)}
    west = {'tilex': lax.rem(me_x + grid_x - 1, grid_x)}
    north = {'tiley': lax.rem(me_y + 1, grid_y)}
    nodes = int_v.shape[0]
    half = halo_v.shape[1] // 2
    quarter = half // 2

    feat_in = []
    for num, (lo, hi) in enumerate(chunks):
        rows = pl.ds(lo, hi - lo)
        feat_in.append(pltpu.make_async_copy(feat_hbm.at[rows, :], feat_v.at[rows, :], feat_sem.at[num]))
        feat_in[-1].start()
    int_in = pltpu.make_async_copy(int_hbm, int_v, int_sem)
    int_in.start()
    halo_in = pltpu.make_async_copy(halo_hbm, halo_v, halo_sem)
    halo_in.start()

    barrier = pltpu.get_barrier_semaphore()
    for neighbour in (north, east, west):
        pl.semaphore_signal(barrier, inc=1, device_id=neighbour, device_id_type=MESH)

    def build_pick(first_buf):
        for buf in (first_buf, first_buf + 1):
            plan = idx_ref[buf:buf + 1, :]

            @pl.loop(0, nodes // N_TILE)
            def _(blk):
                start = pl.multiple_of(blk * N_TILE, N_TILE)
                node_ids = lax.broadcasted_iota(jnp.int32, (N_TILE, quarter), 0) + start
                pick_v[pl.ds(start, N_TILE), buf * quarter:(buf + 1) * quarter] = jnp.where(node_ids == plan, 1.0, 0.0).astype(BF16)

    def remote(src, dst, send_sem, recv_sem, target):
        return pltpu.make_async_remote_copy(src_ref=src, dst_ref=dst, send_sem=send_sem, recv_sem=recv_sem, device_id=target, device_id_type=MESH)

    build_pick(2)
    y_copies = []
    for num, (lo, hi) in enumerate(chunks):
        rows = pl.ds(lo, hi - lo)
        feat_in[num].wait()
        send_y[rows, :] = dot(feat_v[rows, :], pick_v[:, half:], NN).astype(BF16)
        if num == 0:
            pl.semaphore_wait(barrier, 3)
        y_copies.append(remote(send_y.at[rows, :], recv_y.at[rows, :], sy_sem.at[num], ry_sem.at[num], north))
        y_copies[-1].start()
    build_pick(0)
    x_copies = []
    for num, (lo, hi) in enumerate(chunks):
        rows = pl.ds(lo, hi - lo)
        picked = dot(feat_v[rows, :], pick_v[:, :half], NN).astype(BF16)
        send_x0[rows, :] = picked[:, :quarter]
        send_x1[rows, :] = picked[:, quarter:]
        x_copies.append(remote(send_x0.at[rows, :], recv_x.at[rows, :quarter], sx_sem.at[2 * num], rx_sem.at[2 * num], east))
        x_copies.append(remote(send_x1.at[rows, :], recv_x.at[rows, quarter:], sx_sem.at[2 * num + 1], rx_sem.at[2 * num + 1], west))
        x_copies[-2].start()
        x_copies[-1].start()

    int_in.wait()

    @pl.loop(0, nodes // N_TILE)
    def _(blk):
        cols = pl.ds(pl.multiple_of(blk * N_TILE, N_TILE), N_TILE)
        for lo, hi in chunks:
            rows = pl.ds(lo, hi - lo)
            z_int[rows, cols] = dot(feat_v[rows, :], int_v[cols, :], NT)

    halo_in.wait()
    for copy in x_copies:
        copy.wait_recv()

    @pl.loop(0, nodes // N_TILE)
    def _(blk):
        cols = pl.ds(pl.multiple_of(blk * N_TILE, N_TILE), N_TILE)
        for lo, hi in chunks:
            rows = pl.ds(lo, hi - lo)
            z_int[rows, cols] += dot(recv_x[rows, :], halo_v[cols, :half], NT)

    for num, (lo, hi) in enumerate(chunks):
        rows = pl.ds(lo, hi - lo)
        y_copies[num].wait_recv()

        @pl.loop(0, nodes // N_TILE)
        def _(blk):
            cols = pl.ds(pl.multiple_of(blk * N_TILE, N_TILE), N_TILE)
            z_sum = (z_int[rows, cols] + dot(recv_y[rows, :], halo_v[cols, half:], NT)).astype(BF16)
            part = dot(w0_ref[:, lo:hi], z_sum, NN)
            if num == 0:
                hid_acc[:, cols] = part
            else:
                hid_acc[:, cols] += part

    hid_v[...] = jnp.maximum(hid_acc[...], 0.0).astype(BF16)
    hidden = hid_v[...]
    send2_y[...] = dot(hidden, pick_v[:, half:], NN).astype(BF16)
    picked = dot(hidden, pick_v[:, :half], NN).astype(BF16)
    send2_x0[...] = picked[:, :quarter]
    send2_x1[...] = picked[:, quarter:]
    second = [
        remote(send2_y, recv2_y, s2_sem.at[0], r2_sem.at[0], north),
        remote(send2_x0, recv2_x.at[:, :quarter], s2_sem.at[1], r2_sem.at[1], east),
        remote(send2_x1, recv2_x.at[:, quarter:], s2_sem.at[2], r2_sem.at[2], west),
    ]
    for copy in second:
        copy.start()

    @pl.loop(0, nodes // N_TILE)
    def _(blk):
        cols = pl.ds(pl.multiple_of(blk * N_TILE, N_TILE), N_TILE)
        hid_acc[:, cols] = dot(hid_v[...], int_v[cols, :], NT)

    for copy in second:
        copy.wait_recv()

    @pl.loop(0, nodes // N_TILE)
    def _(blk):
        cols = pl.ds(pl.multiple_of(blk * N_TILE, N_TILE), N_TILE)
        z_sum = hid_acc[:, cols] + (dot(recv2_x[...], halo_v[cols, :half], NT) + dot(recv2_y[...], halo_v[cols, half:], NT))
        out_ref[:, cols] = dot(w1_ref[...], z_sum.astype(BF16), NN).astype(BF16)

    for copy in y_copies + x_copies + second:
        copy.wait_send()


def solution(mesh):
    grid_y = mesh.shape['tiley']
    grid_x = mesh.shape['tilex']
    node_spec = P(('parts', 'tiley', 'tilex'), None)
    full_spec = P(None, None)

    def per_device(node_feats, adj_int, adj_halo, send_idx, w_hidden, w_out):
        nodes, feat = node_feats.shape
        slots = adj_halo.shape[1]
        half, quarter = slots // 2, slots // 4
        hidden, classes = w_out.shape
        chunks = feature_chunks(feat)
        vmem = pl.BlockSpec(memory_space=pltpu.VMEM)
        hbm = pl.BlockSpec(memory_space=pl.ANY)
        dma = pltpu.SemaphoreType.DMA
        out = pl.pallas_call(
            functools.partial(gcn_kernel, grid_y, grid_x, chunks),
            out_shape=jax.ShapeDtypeStruct((classes, nodes), BF16),
            in_specs=[vmem, vmem, vmem, hbm, hbm, hbm],
            out_specs=vmem,
            scratch_shapes=[
                pltpu.VMEM((feat, nodes), BF16),
                pltpu.VMEM((nodes, nodes), BF16),
                pltpu.VMEM((nodes, slots), BF16),
                pltpu.VMEM((nodes, slots), BF16),
                pltpu.VMEM((feat, half), BF16),
                pltpu.VMEM((feat, quarter), BF16),
                pltpu.VMEM((feat, quarter), BF16),
                pltpu.VMEM((feat, half), BF16),
                pltpu.VMEM((feat, half), BF16),
                pltpu.VMEM((feat, nodes), F32),
                pltpu.VMEM((hidden, nodes), F32),
                pltpu.VMEM((hidden, nodes), BF16),
                pltpu.VMEM((hidden, half), BF16),
                pltpu.VMEM((hidden, quarter), BF16),
                pltpu.VMEM((hidden, quarter), BF16),
                pltpu.VMEM((hidden, half), BF16),
                pltpu.VMEM((hidden, half), BF16),
                dma((len(chunks),)),
                dma,
                dma,
                dma((len(chunks),)),
                dma((len(chunks),)),
                dma((2 * len(chunks),)),
                dma((2 * len(chunks),)),
                dma((3,)),
                dma((3,)),
            ],
            compiler_params=pltpu.CompilerParams(collective_id=0, has_side_effects=True, vmem_limit_bytes=60 * 2**20),
        )(send_idx, w_hidden.T, w_out.T, node_feats.T, adj_int, adj_halo)
        return out.T

    return jax.shard_map(per_device, mesh=mesh, in_specs=(node_spec, node_spec, node_spec, node_spec, full_spec, full_spec), out_specs=node_spec, check_vma=False)
```

```python
import functools

import jax
import jax.numpy as jnp
from jax import lax
from jax.experimental import pallas as pl
from jax.experimental.pallas import tpu as pltpu
from jax.sharding import PartitionSpec as P

BF16 = jnp.bfloat16
F32 = jnp.float32
MESH = pl.DeviceIdType.MESH
N_TILE = 256
BIG_ROWS = 512
BIG_COLS = 1024
HALO_COLS = 512
NN = (((1,), (0,)), ((), ()))
NT = (((1,), (1,)), ((), ()))


def dot(lhs, rhs, dims):
    return lax.dot_general(lhs, rhs, dims, preferred_element_type=F32)


def feature_chunks(feat):
    cuts = [0, 128]
    while feat - cuts[-1] > 512:
        cuts.append(cuts[-1] + 256)
    if feat - cuts[-1] > 256:
        cuts.append(cuts[-1] + 128)
    cuts.append(feat)
    return list(zip(cuts[:-1], cuts[1:]))


def gcn_kernel(grid_y, grid_x, chunks, idx_ref, w0_ref, w1_ref, feat_hbm, int_hbm, halo_hbm, out_ref,
               feat_v, int_v, halo_v, pick_v, send_y, send_x0, send_x1, recv_y, recv_x, z_int, z_half, hid_acc,
               hid_v, send2_y, send2_x0, send2_x1, recv2_y, recv2_x,
               feat_sem, int_sem, halo_sem, sy_sem, ry_sem, sx_sem, rx_sem, s2_sem, r2_sem):
    me_y = lax.axis_index('tiley')
    me_x = lax.axis_index('tilex')
    east = {'tilex': lax.rem(me_x + 1, grid_x)}
    west = {'tilex': lax.rem(me_x + grid_x - 1, grid_x)}
    north = {'tiley': lax.rem(me_y + 1, grid_y)}
    nodes = int_v.shape[0]
    half = halo_v.shape[1] // 2
    quarter = half // 2

    feat_in = []
    for num, (lo, hi) in enumerate(chunks):
        rows = pl.ds(lo, hi - lo)
        feat_in.append(pltpu.make_async_copy(feat_hbm.at[rows, :], feat_v.at[rows, :], feat_sem.at[num]))
        feat_in[-1].start()
    int_in = pltpu.make_async_copy(int_hbm, int_v, int_sem)
    int_in.start()
    halo_in = pltpu.make_async_copy(halo_hbm, halo_v, halo_sem)
    halo_in.start()

    barrier = pltpu.get_barrier_semaphore()
    for neighbour in (north, east, west):
        pl.semaphore_signal(barrier, inc=1, device_id=neighbour, device_id_type=MESH)

    def build_pick(first_buf):
        for buf in (first_buf, first_buf + 1):
            plan = idx_ref[buf:buf + 1, :]

            @pl.loop(0, nodes // N_TILE)
            def _(blk):
                start = pl.multiple_of(blk * N_TILE, N_TILE)
                node_ids = lax.broadcasted_iota(jnp.int32, (N_TILE, quarter), 0) + start
                pick_v[pl.ds(start, N_TILE), buf * quarter:(buf + 1) * quarter] = jnp.where(node_ids == plan, 1.0, 0.0).astype(BF16)

    def remote(src, dst, send_sem, recv_sem, target):
        return pltpu.make_async_remote_copy(src_ref=src, dst_ref=dst, send_sem=send_sem, recv_sem=recv_sem, device_id=target, device_id_type=MESH)

    with jax.named_scope('pick_y'):
        build_pick(2)
    y_copies = []
    x_copies = []

    def send_y_rows(num, rows):
        y_copies.append(remote(send_y.at[rows, :], recv_y.at[rows, :], sy_sem.at[num], ry_sem.at[num], north))
        y_copies[-1].start()

    def send_x_rows(num, rows):
        x_copies.append(remote(send_x0.at[rows, :], recv_x.at[rows, :quarter], sx_sem.at[2 * num], rx_sem.at[2 * num], east))
        x_copies.append(remote(send_x1.at[rows, :], recv_x.at[rows, quarter:], sx_sem.at[2 * num + 1], rx_sem.at[2 * num + 1], west))
        x_copies[-2].start()
        x_copies[-1].start()

    for num, (lo, hi) in enumerate(chunks):
        rows = pl.ds(lo, hi - lo)
        with jax.named_scope(f'feat_wait{num}'):
            feat_in[num].wait()
        with jax.named_scope(f'gather_y{num}'):
            send_y[rows, :] = dot(feat_v[rows, :], pick_v[:, half:], NN).astype(BF16)
        if num == 0:
            with jax.named_scope('barrier'):
                pl.semaphore_wait(barrier, 3)
        send_y_rows(num, rows)
        if num == 0:
            with jax.named_scope('pick_x'):
                build_pick(0)
        with jax.named_scope(f'gather_x{num}'):
            picked = dot(feat_v[rows, :], pick_v[:, :half], NN).astype(BF16)
            send_x0[rows, :] = picked[:, :quarter]
            send_x1[rows, :] = picked[:, quarter:]
        send_x_rows(num, rows)

    with jax.named_scope('int_wait'):
        int_in.wait()
    big = [(lo, min(lo + BIG_ROWS, feat_v.shape[0])) for lo in range(0, feat_v.shape[0], BIG_ROWS)]
    with jax.named_scope('interior'):

        @pl.loop(0, nodes // BIG_COLS)
        def _(blk):
            cols = pl.ds(pl.multiple_of(blk * BIG_COLS, BIG_COLS), BIG_COLS)
            for lo, hi in big:
                z_int[lo:hi, cols] = dot(feat_v[lo:hi, :], int_v[cols, :], NT)

    with jax.named_scope('xwait'):
        halo_in.wait()
        for copy in x_copies:
            copy.wait_recv()
    with jax.named_scope('xhalo'):

        @pl.loop(0, nodes // BIG_COLS)
        def _(blk):
            cols = pl.ds(pl.multiple_of(blk * BIG_COLS, BIG_COLS), BIG_COLS)
            for lo, hi in big:
                z_int[lo:hi, cols] += dot(recv_x[lo:hi, :], halo_v[cols, :half], NT)

    for num, (lo, hi) in enumerate(chunks):
        rows = pl.ds(lo, hi - lo)
        with jax.named_scope(f'ywait{num}'):
            y_copies[num].wait_recv()
        with jax.named_scope(f'yhalo{num}'):
            for col in range(0, nodes, HALO_COLS):
                cols = pl.ds(col, HALO_COLS)
                z_half[rows, cols] = (z_int[rows, cols] + dot(recv_y[rows, :], halo_v[cols, half:], NT)).astype(BF16)
            part = dot(w0_ref[:, lo:hi], z_half[rows, :], NN)
            if num == 0:
                hid_acc[...] = part
            else:
                hid_acc[...] += part

    with jax.named_scope('gather2'):
        hidden = jnp.maximum(hid_acc[...], 0.0).astype(BF16)
        hid_v[...] = hidden
        send2_y[...] = dot(hidden, pick_v[:, half:], NN).astype(BF16)
        picked = dot(hidden, pick_v[:, :half], NN).astype(BF16)
        send2_x0[...] = picked[:, :quarter]
        send2_x1[...] = picked[:, quarter:]
        second = [
            remote(send2_y, recv2_y, s2_sem.at[0], r2_sem.at[0], north),
            remote(send2_x0, recv2_x.at[:, :quarter], s2_sem.at[1], r2_sem.at[1], east),
            remote(send2_x1, recv2_x.at[:, quarter:], s2_sem.at[2], r2_sem.at[2], west),
        ]
        for copy in second:
            copy.start()

    with jax.named_scope('interior2'):
        hid_acc[...] = dot(hid_v[...], int_v[...], NT)
    with jax.named_scope('wait2'):
        for copy in second:
            copy.wait_recv()
    with jax.named_scope('halo2'):
        z_sum = hid_acc[...] + (dot(recv2_x[...], halo_v[:, :half], NT) + dot(recv2_y[...], halo_v[:, half:], NT))
        out_ref[...] = dot(w1_ref[...], z_sum.astype(BF16), NN).astype(BF16)
    with jax.named_scope('sendwait'):
        for copy in y_copies + x_copies + second:
            copy.wait_send()


def solution(mesh):
    grid_y = mesh.shape['tiley']
    grid_x = mesh.shape['tilex']
    node_spec = P(('parts', 'tiley', 'tilex'), None)
    full_spec = P(None, None)

    def per_device(node_feats, adj_int, adj_halo, send_idx, w_hidden, w_out):
        nodes, feat = node_feats.shape
        slots = adj_halo.shape[1]
        half, quarter = slots // 2, slots // 4
        hidden, classes = w_out.shape
        chunks = feature_chunks(feat)
        vmem = pl.BlockSpec(memory_space=pltpu.VMEM)
        hbm = pl.BlockSpec(memory_space=pl.ANY)
        dma = pltpu.SemaphoreType.DMA
        out = pl.pallas_call(
            functools.partial(gcn_kernel, grid_y, grid_x, chunks),
            out_shape=jax.ShapeDtypeStruct((classes, nodes), BF16),
            in_specs=[vmem, vmem, vmem, hbm, hbm, hbm],
            out_specs=vmem,
            scratch_shapes=[
                pltpu.VMEM((feat, nodes), BF16),
                pltpu.VMEM((nodes, nodes), BF16),
                pltpu.VMEM((nodes, slots), BF16),
                pltpu.VMEM((nodes, slots), BF16),
                pltpu.VMEM((feat, half), BF16),
                pltpu.VMEM((feat, quarter), BF16),
                pltpu.VMEM((feat, quarter), BF16),
                pltpu.VMEM((feat, half), BF16),
                pltpu.VMEM((feat, half), BF16),
                pltpu.VMEM((feat, nodes), F32),
                pltpu.VMEM((feat, nodes), BF16),
                pltpu.VMEM((hidden, nodes), F32),
                pltpu.VMEM((hidden, nodes), BF16),
                pltpu.VMEM((hidden, half), BF16),
                pltpu.VMEM((hidden, quarter), BF16),
                pltpu.VMEM((hidden, quarter), BF16),
                pltpu.VMEM((hidden, half), BF16),
                pltpu.VMEM((hidden, half), BF16),
                dma((len(chunks),)),
                dma,
                dma,
                dma((len(chunks),)),
                dma((len(chunks),)),
                dma((2 * len(chunks),)),
                dma((2 * len(chunks),)),
                dma((3,)),
                dma((3,)),
            ],
            compiler_params=pltpu.CompilerParams(collective_id=0, has_side_effects=True, vmem_limit_bytes=60 * 2**20),
        )(send_idx, w_hidden.T, w_out.T, node_feats.T, adj_int, adj_halo)
        return out.T

    return jax.shard_map(per_device, mesh=mesh, in_specs=(node_spec, node_spec, node_spec, node_spec, full_spec, full_spec), out_specs=node_spec, check_vma=False)
```

```python
import functools

import jax
import jax.numpy as jnp
from jax import lax
from jax.experimental import pallas as pl
from jax.experimental.pallas import tpu as pltpu
from jax.sharding import PartitionSpec as P

BF16 = jnp.bfloat16
F32 = jnp.float32
MESH = pl.DeviceIdType.MESH
N_TILE = 256
BIG_ROWS = 512
BIG_COLS = 1024
HALO_COLS = 512
NN = (((1,), (0,)), ((), ()))
NT = (((1,), (1,)), ((), ()))


def dot(lhs, rhs, dims):
    return lax.dot_general(lhs, rhs, dims, preferred_element_type=F32)


def feature_chunks(feat):
    cuts = [0, 128]
    while feat - cuts[-1] > 512:
        cuts.append(cuts[-1] + 256)
    if feat - cuts[-1] > 256:
        cuts.append(cuts[-1] + 128)
    cuts.append(feat)
    return list(zip(cuts[:-1], cuts[1:]))


def gcn_kernel(grid_y, grid_x, chunks, idx_hbm, w0_hbm, w1_hbm, feat_hbm, int_hbm, halo_hbm, out_ref,
               idx_ref, w0_ref, w1_ref, feat_v, int_v, halo_v, halo_t, pick_v, send_y, send_x0, send_x1, recv_y, recv_x, z_int, z_half, hid_acc,
               hid_v, send2_y, send2_x0, send2_x1, recv2_y, recv2_x,
               small_sem, feat_sem, int_sem, halo_sem, sy_sem, ry_sem, sx_sem, rx_sem, s2_sem, r2_sem):
    me_y = lax.axis_index('tiley')
    me_x = lax.axis_index('tilex')
    east = {'tilex': lax.rem(me_x + 1, grid_x)}
    west = {'tilex': lax.rem(me_x + grid_x - 1, grid_x)}
    north = {'tiley': lax.rem(me_y + 1, grid_y)}
    nodes = int_v.shape[0]
    half = halo_v.shape[1] // 2
    quarter = half // 2

    barrier = pltpu.get_barrier_semaphore()
    for neighbour in (north, east, west):
        pl.semaphore_signal(barrier, inc=1, device_id=neighbour, device_id_type=MESH)

    idx_in = pltpu.make_async_copy(idx_hbm, idx_ref, small_sem.at[0])
    feat_in = []
    for num, (lo, hi) in enumerate(chunks):
        rows = pl.ds(lo, hi - lo)
        feat_in.append(pltpu.make_async_copy(feat_hbm.at[rows, :], feat_v.at[rows, :], feat_sem.at[num]))
    w0_in = pltpu.make_async_copy(w0_hbm, w0_ref, small_sem.at[1])
    w1_in = pltpu.make_async_copy(w1_hbm, w1_ref, small_sem.at[2])
    int_in = pltpu.make_async_copy(int_hbm, int_v, int_sem)
    halo_in = pltpu.make_async_copy(halo_hbm, halo_v, halo_sem)
    idx_in.start()
    feat_in[0].start()

    def pick_block(buf, start):
        node_ids = lax.broadcasted_iota(jnp.int32, (N_TILE, quarter), 0) + start
        return jnp.where(node_ids == idx_ref[buf:buf + 1, :], 1.0, 0.0).astype(BF16)

    def build_pick(first_buf):
        for buf in (first_buf, first_buf + 1):

            @pl.loop(0, nodes // N_TILE)
            def _(blk):
                start = pl.multiple_of(blk * N_TILE, N_TILE)
                pick_v[pl.ds(start, N_TILE), buf * quarter:(buf + 1) * quarter] = pick_block(buf, start)

    def remote(src, dst, send_sem, recv_sem, target):
        return pltpu.make_async_remote_copy(src_ref=src, dst_ref=dst, send_sem=send_sem, recv_sem=recv_sem, device_id=target, device_id_type=MESH)

    with jax.named_scope('idx_wait'):
        idx_in.wait()
    for copy in feat_in[1:]:
        copy.start()
    y_copies = []
    x_copies = []

    def send_y_rows(num, rows):
        y_copies.append(remote(send_y.at[rows, :], recv_y.at[rows, :], sy_sem.at[num], ry_sem.at[num], north))
        y_copies[-1].start()

    def send_x_rows(num, rows):
        x_copies.append(remote(send_x0.at[rows, :], recv_x.at[rows, :quarter], sx_sem.at[2 * num], rx_sem.at[2 * num], east))
        x_copies.append(remote(send_x1.at[rows, :], recv_x.at[rows, quarter:], sx_sem.at[2 * num + 1], rx_sem.at[2 * num + 1], west))
        x_copies[-2].start()
        x_copies[-1].start()

    for num, (lo, hi) in enumerate(chunks):
        rows = pl.ds(lo, hi - lo)
        with jax.named_scope(f'feat_wait{num}'):
            feat_in[num].wait()
        with jax.named_scope(f'gather_y{num}'):
            if num == 0:
                picked = None
                for start in range(0, nodes, N_TILE):
                    block = jnp.concatenate([pick_block(2, start), pick_block(3, start)], axis=1)
                    pick_v[start:start + N_TILE, half:] = block
                    part = dot(feat_v[rows, start:start + N_TILE], block, NN)
                    picked = part if picked is None else picked + part
                send_y[rows, :] = picked.astype(BF16)
            else:
                send_y[rows, :] = dot(feat_v[rows, :], pick_v[:, half:], NN).astype(BF16)
        if num == 0:
            with jax.named_scope('barrier'):
                pl.semaphore_wait(barrier, 3)
        send_y_rows(num, rows)
        if num == 0:
            for copy in (int_in, halo_in, w0_in, w1_in):
                copy.start()
            with jax.named_scope('pick_x'):
                build_pick(0)
        with jax.named_scope(f'gather_x{num}'):
            picked = dot(feat_v[rows, :], pick_v[:, :half], NN).astype(BF16)
            send_x0[rows, :] = picked[:, :quarter]
            send_x1[rows, :] = picked[:, quarter:]
        send_x_rows(num, rows)

    with jax.named_scope('int_wait'):
        int_in.wait()
        halo_in.wait()
        w0_in.wait()
        w1_in.wait()
    big = [(lo, min(lo + BIG_ROWS, feat_v.shape[0])) for lo in range(0, feat_v.shape[0], BIG_ROWS)]
    with jax.named_scope('interior'):

        @pl.loop(0, nodes // BIG_COLS)
        def _(blk):
            cols = pl.ds(pl.multiple_of(blk * BIG_COLS, BIG_COLS), BIG_COLS)
            halo_t[:, cols] = halo_v[cols, :].T
            for lo, hi in big:
                z_int[lo:hi, cols] = dot(feat_v[lo:hi, :], int_v[cols, :], NT)

    with jax.named_scope('xwait'):
        for copy in x_copies:
            copy.wait_recv()
    with jax.named_scope('xhalo'):

        @pl.loop(0, nodes // BIG_COLS)
        def _(blk):
            cols = pl.ds(pl.multiple_of(blk * BIG_COLS, BIG_COLS), BIG_COLS)
            for lo, hi in big:
                z_int[lo:hi, cols] += dot(recv_x[lo:hi, :], halo_v[cols, :half], NT)

    for num, (lo, hi) in enumerate(chunks):
        rows = pl.ds(lo, hi - lo)
        with jax.named_scope(f'ywait{num}'):
            y_copies[num].wait_recv()
        with jax.named_scope(f'yhalo{num}'):
            for col in range(0, nodes, HALO_COLS):
                cols = pl.ds(col, HALO_COLS)
                z_half[rows, cols] = (z_int[rows, cols] + dot(recv_y[rows, :], halo_t[half:, cols], NN)).astype(BF16)
            part = dot(w0_ref[:, lo:hi], z_half[rows, :], NN)
            if num == 0:
                hid_acc[...] = part
            else:
                hid_acc[...] += part

    with jax.named_scope('gather2'):
        hidden = jnp.maximum(hid_acc[...], 0.0).astype(BF16)
        hid_v[...] = hidden
        send2_y[...] = dot(hidden, pick_v[:, half:], NN).astype(BF16)
        picked = dot(hidden, pick_v[:, :half], NN).astype(BF16)
        send2_x0[...] = picked[:, :quarter]
        send2_x1[...] = picked[:, quarter:]
        second = [
            remote(send2_y, recv2_y, s2_sem.at[0], r2_sem.at[0], north),
            remote(send2_x0, recv2_x.at[:, :quarter], s2_sem.at[1], r2_sem.at[1], east),
            remote(send2_x1, recv2_x.at[:, quarter:], s2_sem.at[2], r2_sem.at[2], west),
        ]
        for copy in second:
            copy.start()

    with jax.named_scope('interior2'):
        hid_acc[...] = dot(hid_v[...], int_v[...], NT)
    with jax.named_scope('wait2'):
        for copy in second:
            copy.wait_recv()
    with jax.named_scope('halo2'):
        z_sum = hid_acc[...] + (dot(recv2_x[...], halo_t[:half, :], NN) + dot(recv2_y[...], halo_t[half:, :], NN))
        out_ref[...] = dot(w1_ref[...], z_sum.astype(BF16), NN).astype(BF16)
    with jax.named_scope('sendwait'):
        for copy in y_copies + x_copies + second:
            copy.wait_send()


def solution(mesh):
    grid_y = mesh.shape['tiley']
    grid_x = mesh.shape['tilex']
    node_spec = P(('parts', 'tiley', 'tilex'), None)
    full_spec = P(None, None)

    def per_device(node_feats, adj_int, adj_halo, send_idx, w_hidden, w_out):
        nodes, feat = node_feats.shape
        slots = adj_halo.shape[1]
        half, quarter = slots // 2, slots // 4
        hidden, classes = w_out.shape
        chunks = feature_chunks(feat)
        vmem = pl.BlockSpec(memory_space=pltpu.VMEM)
        hbm = pl.BlockSpec(memory_space=pl.ANY)
        dma = pltpu.SemaphoreType.DMA
        out = pl.pallas_call(
            functools.partial(gcn_kernel, grid_y, grid_x, chunks),
            out_shape=pltpu.VMEM((classes, nodes), BF16),
            in_specs=[hbm] * 6,
            out_specs=vmem,
            scratch_shapes=[
                pltpu.VMEM(send_idx.shape, jnp.int32),
                pltpu.VMEM((hidden, feat), BF16),
                pltpu.VMEM((classes, hidden), BF16),
                pltpu.VMEM((feat, nodes), BF16),
                pltpu.VMEM((nodes, nodes), BF16),
                pltpu.VMEM((nodes, slots), BF16),
                pltpu.VMEM((slots, nodes), BF16),
                pltpu.VMEM((nodes, slots), BF16),
                pltpu.VMEM((feat, half), BF16),
                pltpu.VMEM((feat, quarter), BF16),
                pltpu.VMEM((feat, quarter), BF16),
                pltpu.VMEM((feat, half), BF16),
                pltpu.VMEM((feat, half), BF16),
                pltpu.VMEM((feat, nodes), F32),
                pltpu.VMEM((feat, nodes), BF16),
                pltpu.VMEM((hidden, nodes), F32),
                pltpu.VMEM((hidden, nodes), BF16),
                pltpu.VMEM((hidden, half), BF16),
                pltpu.VMEM((hidden, quarter), BF16),
                pltpu.VMEM((hidden, quarter), BF16),
                pltpu.VMEM((hidden, half), BF16),
                pltpu.VMEM((hidden, half), BF16),
                dma((3,)),
                dma((len(chunks),)),
                dma,
                dma,
                dma((len(chunks),)),
                dma((len(chunks),)),
                dma((2 * len(chunks),)),
                dma((2 * len(chunks),)),
                dma((3,)),
                dma((3,)),
            ],
            compiler_params=pltpu.CompilerParams(collective_id=0, has_side_effects=True, vmem_limit_bytes=60 * 2**20),
        )(send_idx, w_hidden.T, w_out.T, node_feats.T, adj_int, adj_halo)
        return out.T

    return jax.shard_map(per_device, mesh=mesh, in_specs=(node_spec, node_spec, node_spec, node_spec, full_spec, full_spec), out_specs=node_spec, check_vma=False)
```

```python
import functools

import jax
import jax.numpy as jnp
from jax import lax
from jax.experimental import pallas as pl
from jax.experimental.pallas import tpu as pltpu
from jax.sharding import PartitionSpec as P

BF16 = jnp.bfloat16
F32 = jnp.float32
MESH = pl.DeviceIdType.MESH
N_TILE = 256
BIG_ROWS = 512
LAST_ROWS = 96
BIG_COLS = 1024
HALO_COLS = 512
NN = (((1,), (0,)), ((), ()))
NT = (((1,), (1,)), ((), ()))


def dot(lhs, rhs, dims):
    return lax.dot_general(lhs, rhs, dims, preferred_element_type=F32)


def feature_chunks(feat):
    last = (feat - 80) // 64 * 64
    cuts = [0, 64, 256]
    while last - 128 - cuts[-1] > 256:
        cuts.append(cuts[-1] + 256)
    cuts += [last - 128, last, feat]
    return list(zip(cuts[:-1], cuts[1:]))


def big_chunks(feat):
    return [(lo, min(lo + BIG_ROWS, feat)) for lo in range(0, feat, BIG_ROWS)]


def gcn_kernel(grid_y, grid_x, chunks, big, idx_hbm, w0_hbm, w1_hbm, feat_hbm, int_hbm, halo_hbm, out_ref,
               idx_ref, w0_ref, w1_ref, feat_v, int_v, int_t, halo_v, halo_t, pick_v, send_y, send_x0, send_x1, recv_v, z_int, z_half, halo_pick, z_split, z_pick, hid_split, hid_pick, hid_acc,
               hid_v, send2_y, send2_x0, send2_x1, recv2_y, recv2_x,
               small_sem, feat_sem, int_sem, halo_sem, sy_sem, ry_sem, sx_sem, rx_sem, s2_sem, r2_sem):
    me_y = lax.axis_index('tiley')
    me_x = lax.axis_index('tilex')
    east = {'tilex': lax.rem(me_x + 1, grid_x)}
    west = {'tilex': lax.rem(me_x + grid_x - 1, grid_x)}
    north = {'tiley': lax.rem(me_y + 1, grid_y)}
    nodes = int_v.shape[0]
    half = halo_v.shape[1] // 2
    quarter = half // 2
    hid_rows = hid_v.shape[0]

    barrier = pltpu.get_barrier_semaphore()
    for neighbour in (north, east, west):
        pl.semaphore_signal(barrier, inc=1, device_id=neighbour, device_id_type=MESH)

    idx_in = pltpu.make_async_copy(idx_hbm, idx_ref, small_sem.at[0])
    feat_in = []
    for num, (lo, hi) in enumerate(chunks):
        rows = pl.ds(lo, hi - lo)
        feat_in.append(pltpu.make_async_copy(feat_hbm.at[rows, :], feat_v.at[rows, :], feat_sem.at[num]))
    w0_in = pltpu.make_async_copy(w0_hbm, w0_ref, small_sem.at[1])
    w1_in = pltpu.make_async_copy(w1_hbm, w1_ref, small_sem.at[2])
    int_in = pltpu.make_async_copy(int_hbm, int_v, int_sem)
    halo_in = pltpu.make_async_copy(halo_hbm, halo_v, halo_sem)
    idx_in.start()
    feat_in[0].start()

    def pick_block(buf, start):
        node_ids = lax.broadcasted_iota(jnp.int32, (N_TILE, quarter), 0) + start
        return jnp.where(node_ids == idx_ref[buf:buf + 1, :], 1.0, 0.0).astype(BF16)

    def build_pick(first_buf):
        @pl.loop(0, nodes // N_TILE)
        def _(blk):
            start = pl.multiple_of(blk * N_TILE, N_TILE)
            for buf in (first_buf, first_buf + 1):
                pick_v[pl.ds(start, N_TILE), buf * quarter:(buf + 1) * quarter] = pick_block(buf, start)

    def remote(src, dst, send_sem, recv_sem, target):
        return pltpu.make_async_remote_copy(src_ref=src, dst_ref=dst, send_sem=send_sem, recv_sem=recv_sem, device_id=target, device_id_type=MESH)

    with jax.named_scope('idx_wait'):
        idx_in.wait()
    for copy in feat_in[1:]:
        copy.start()
    y_copies = []
    x_copies = []

    def send_y_rows(first, end):
        lo, hi = chunks[first][0], chunks[end - 1][1]
        rows = pl.ds(lo, hi - lo)
        with jax.named_scope(f'feat_wait{first}'):
            for copy in feat_in[first:end]:
                copy.wait()
        with jax.named_scope(f'gather_y{first}'):
            if first == 0:
                picked = None
                for start in range(0, nodes, N_TILE):
                    block = jnp.concatenate([pick_block(2, start), pick_block(3, start)], axis=1)
                    pick_v[start:start + N_TILE, half:] = block
                    part = dot(feat_v[rows, start:start + N_TILE], block, NN)
                    picked = part if picked is None else picked + part
                send_y[rows, :] = picked.astype(BF16)
            else:
                send_y[rows, :] = dot(feat_v[rows, :], pick_v[:, half:], NN).astype(BF16)
        if first == 0:
            with jax.named_scope('barrier'):
                pl.semaphore_wait(barrier, 3)
        for num in range(first, end):
            rows = pl.ds(chunks[num][0], chunks[num][1] - chunks[num][0])
            y_copies.append(remote(send_y.at[rows, :], recv_v.at[rows, half:], sy_sem.at[num], ry_sem.at[num], north))
            y_copies[-1].start()

    def send_x_rows(num):
        rows = pl.ds(big[num][0], big[num][1] - big[num][0])
        with jax.named_scope(f'gather_x{num}'):
            picked = dot(feat_v[rows, :], pick_v[:, :half], NN).astype(BF16)
            send_x0[rows, :] = picked[:, :quarter]
            send_x1[rows, :] = picked[:, quarter:]
        x_copies.append(remote(send_x0.at[rows, :], recv_v.at[rows, :quarter], sx_sem.at[2 * num], rx_sem.at[2 * num], east))
        x_copies.append(remote(send_x1.at[rows, :], recv_v.at[rows, quarter:half], sx_sem.at[2 * num + 1], rx_sem.at[2 * num + 1], west))
        x_copies[-2].start()
        x_copies[-1].start()

    next_x = 0
    for first, end in [(0, 1), (1, 2), (2, 4), (4, len(chunks))]:
        send_y_rows(first, end)
        if first == 0:
            for copy in (int_in, halo_in, w0_in, w1_in):
                copy.start()
        if first == 1:
            with jax.named_scope('pick_x'):
                build_pick(0)
        while next_x < len(big) and big[next_x][1] <= chunks[end - 1][1]:
            send_x_rows(next_x)
            next_x += 1

    with jax.named_scope('int_wait'):
        int_in.wait()
        halo_in.wait()
        w0_in.wait()
        w1_in.wait()
    with jax.named_scope('interior'):

        @pl.loop(0, nodes // BIG_COLS)
        def _(blk):
            cols = pl.ds(pl.multiple_of(blk * BIG_COLS, BIG_COLS), BIG_COLS)
            halo_t[:, cols] = halo_v[cols, :].T
            int_t[:, cols] = int_v[cols, :].T
            for lo, hi in big:
                z_int[lo:hi, cols] = dot(feat_v[lo:hi, :], int_v[cols, :], NT)

    with jax.named_scope('xwait'):
        for copy in x_copies:
            copy.wait_recv()
    def split3(value):
        high = value.astype(BF16)
        rest = value - high.astype(F32)
        middle = rest.astype(BF16)
        return high, middle, (rest - middle.astype(F32)).astype(BF16)

    last_lo, last_hi = chunks[-1]
    last = pl.ds(last_lo, last_hi - last_lo)
    tail = last_hi - last_lo
    with jax.named_scope('halo_pick'):
        halo_pick[...] = dot(halo_t[half:, :], pick_v[...], NN).astype(BF16)
    with jax.named_scope('last_x'):
        z_last = z_int[last, :] + dot(recv_v[last, :half], halo_t[:half, :], NN)
        z_int[last, :] = z_last
        for num, piece in enumerate(split3(z_last)):
            z_split[num * LAST_ROWS:num * LAST_ROWS + tail, :] = piece
    with jax.named_scope('last_pick'):
        parts = dot(z_split[...], pick_v[...], NN)
        z_pick[...] = parts[:LAST_ROWS] + parts[LAST_ROWS:2 * LAST_ROWS] + parts[2 * LAST_ROWS:]

    groups = [(0, 3)] + [(num, num + 1) for num in range(3, len(chunks) - 1)]
    for first, end in groups:
        lo, hi = chunks[first][0], chunks[end - 1][1]
        with jax.named_scope(f'ywait{first}'):
            for copy in y_copies[first:end]:
                copy.wait_recv()
        rows = pl.ds(lo, hi - lo)
        with jax.named_scope(f'yhalo{first}'):
            for col in range(0, nodes, HALO_COLS):
                cols = pl.ds(col, HALO_COLS)
                z_half[:hi - lo, cols] = (z_int[rows, cols] + dot(recv_v[rows, :], halo_t[:, cols], NN)).astype(BF16)
            part = dot(w0_ref[:, lo:hi], z_half[:hi - lo, :], NN)
            if first == 0:
                hid_acc[...] = part
            else:
                hid_acc[...] += part
    with jax.named_scope('hid_pick'):
        for num, piece in enumerate(split3(hid_acc[...])):
            hid_split[num * hid_rows:(num + 1) * hid_rows, :] = piece
        parts = dot(hid_split[...], pick_v[...], NN)
        hid_pick[...] = parts[:hid_rows] + parts[hid_rows:2 * hid_rows] + parts[2 * hid_rows:]

    second = [
        remote(send2_y, recv2_y, s2_sem.at[0], r2_sem.at[0], north),
        remote(send2_x0, recv2_x.at[:, :quarter], s2_sem.at[1], r2_sem.at[1], east),
        remote(send2_x1, recv2_x.at[:, quarter:], s2_sem.at[2], r2_sem.at[2], west),
    ]
    with jax.named_scope('ywait_last'):
        y_copies[-1].wait_recv()
    with jax.named_scope('sent2'):
        z_sent = (z_pick[:tail, :] + dot(recv_v[last, half:], halo_pick[...], NN)).astype(BF16)
        sent = hid_pick[...] + dot(w0_ref[:, last_lo:last_hi], z_sent, NN)
        sent = jnp.maximum(sent, 0.0).astype(BF16)
        send2_y[...] = sent[:, half:]
        send2_x0[...] = sent[:, :quarter]
        send2_x1[...] = sent[:, quarter:half]
    for copy in second:
        copy.start()
    with jax.named_scope('yhalo_last'):
        z_sum = (z_int[last, :] + dot(recv_v[last, half:], halo_t[half:, :], NN)).astype(BF16)
        hid_sum = hid_acc[...] + dot(w0_ref[:, last_lo:last_hi], z_sum, NN)
        hid_v[...] = jnp.maximum(hid_sum, 0.0).astype(BF16)
    with jax.named_scope('interior2'):
        hid_acc[...] = dot(hid_v[...], int_t[...], NN)
    with jax.named_scope('wait2x'):
        second[1].wait_recv()
        second[2].wait_recv()
    with jax.named_scope('xhalo2'):
        hid_acc[...] += dot(recv2_x[...], halo_t[:half, :], NN)
    with jax.named_scope('wait2y'):
        second[0].wait_recv()
    with jax.named_scope('yhalo2'):
        z_sum = hid_acc[...] + dot(recv2_y[...], halo_t[half:, :], NN)
        out_ref[...] = dot(w1_ref[...], z_sum.astype(BF16), NN).astype(BF16)
    with jax.named_scope('sendwait'):
        for copy in y_copies + x_copies + second:
            copy.wait_send()


def solution(mesh):
    grid_y = mesh.shape['tiley']
    grid_x = mesh.shape['tilex']
    node_spec = P(('parts', 'tiley', 'tilex'), None)
    full_spec = P(None, None)

    def per_device(node_feats, adj_int, adj_halo, send_idx, w_hidden, w_out):
        nodes, feat = node_feats.shape
        slots = adj_halo.shape[1]
        half, quarter = slots // 2, slots // 4
        hidden, classes = w_out.shape
        chunks = feature_chunks(feat)
        big = big_chunks(feat)
        vmem = pl.BlockSpec(memory_space=pltpu.VMEM)
        hbm = pl.BlockSpec(memory_space=pl.ANY)
        dma = pltpu.SemaphoreType.DMA
        out = pl.pallas_call(
            functools.partial(gcn_kernel, grid_y, grid_x, chunks, big),
            out_shape=pltpu.VMEM((classes, nodes), BF16),
            in_specs=[hbm] * 6,
            out_specs=vmem,
            scratch_shapes=[
                pltpu.VMEM(send_idx.shape, jnp.int32),
                pltpu.VMEM((hidden, feat), BF16),
                pltpu.VMEM((classes, hidden), BF16),
                pltpu.VMEM((feat, nodes), BF16),
                pltpu.VMEM((nodes, nodes), BF16),
                pltpu.VMEM((nodes, nodes), BF16),
                pltpu.VMEM((nodes, slots), BF16),
                pltpu.VMEM((slots, nodes), BF16),
                pltpu.VMEM((nodes, slots), BF16),
                pltpu.VMEM((feat, half), BF16),
                pltpu.VMEM((feat, quarter), BF16),
                pltpu.VMEM((feat, quarter), BF16),
                pltpu.VMEM((feat, slots), BF16),
                pltpu.VMEM((feat, nodes), F32),
                pltpu.VMEM((512, nodes), BF16),
                pltpu.VMEM((half, slots), BF16),
                pltpu.VMEM((3 * LAST_ROWS, nodes), BF16),
                pltpu.VMEM((LAST_ROWS, slots), F32),
                pltpu.VMEM((3 * hidden, nodes), BF16),
                pltpu.VMEM((hidden, slots), F32),
                pltpu.VMEM((hidden, nodes), F32),
                pltpu.VMEM((hidden, nodes), BF16),
                pltpu.VMEM((hidden, half), BF16),
                pltpu.VMEM((hidden, quarter), BF16),
                pltpu.VMEM((hidden, quarter), BF16),
                pltpu.VMEM((hidden, half), BF16),
                pltpu.VMEM((hidden, half), BF16),
                dma((3,)),
                dma((len(chunks),)),
                dma,
                dma,
                dma((len(chunks),)),
                dma((len(chunks),)),
                dma((2 * len(big),)),
                dma((2 * len(big),)),
                dma((3,)),
                dma((3,)),
            ],
            compiler_params=pltpu.CompilerParams(collective_id=0, has_side_effects=True, vmem_limit_bytes=60 * 2**20),
        )(send_idx, w_hidden.T, w_out.T, node_feats.T, adj_int, adj_halo)
        return out.T

    return jax.shard_map(per_device, mesh=mesh, in_specs=(node_spec, node_spec, node_spec, node_spec, full_spec, full_spec), out_specs=node_spec, check_vma=False)
```

```python
import functools

import jax
import jax.numpy as jnp
from jax import lax
from jax.experimental import pallas as pl
from jax.experimental.pallas import tpu as pltpu
from jax.sharding import PartitionSpec as P

BF16 = jnp.bfloat16
F32 = jnp.float32
MESH = pl.DeviceIdType.MESH
N_TILE = 256
BIG_ROWS = 512
LAST_ROWS = 128
BIG_COLS = 1024
HALO_COLS = 512
NN = (((1,), (0,)), ((), ()))
NT = (((1,), (1,)), ((), ()))


def dot(lhs, rhs, dims):
    return lax.dot_general(lhs, rhs, dims, preferred_element_type=F32)


def feature_chunks(feat):
    last = (feat - 112) // 16 * 16
    cuts = [0, 64, 256]
    while last - 128 - cuts[-1] > 256:
        cuts.append(cuts[-1] + 256)
    cuts += [last - 128, last, feat]
    return list(zip(cuts[:-1], cuts[1:]))


def big_chunks(feat):
    return [(lo, min(lo + BIG_ROWS, feat)) for lo in range(0, feat, BIG_ROWS)]


def x_chunks(feat):
    return [(0, BIG_ROWS), (BIG_ROWS, feat)]


def gcn_kernel(grid_y, grid_x, chunks, x_parts, big, idx_hbm, w0_hbm, w1_hbm, feat_hbm, int_hbm, halo_hbm, out_ref,
               idx_ref, w0_ref, w1_ref, feat_v, int_v, int_t, halo_v, halo_t, pick_v, send_y, send_x0, send_x1, recv_v, z_int, z_half, halo_pick, z_split, z_pick, hid_split, hid_pick, hid_acc,
               hid_v, send2_y, send2_x0, send2_x1, recv2_y, recv2_x,
               small_sem, feat_sem, int_sem, halo_sem, sy_sem, ry_sem, sx_sem, rx_sem, s2_sem, r2_sem):
    me_y = lax.axis_index('tiley')
    me_x = lax.axis_index('tilex')
    east = {'tilex': lax.rem(me_x + 1, grid_x)}
    west = {'tilex': lax.rem(me_x + grid_x - 1, grid_x)}
    north = {'tiley': lax.rem(me_y + 1, grid_y)}
    nodes = int_v.shape[0]
    half = halo_v.shape[1] // 2
    quarter = half // 2
    hid_rows = hid_v.shape[0]

    barrier = pltpu.get_barrier_semaphore()
    for neighbour in (north, east, west):
        pl.semaphore_signal(barrier, inc=1, device_id=neighbour, device_id_type=MESH)

    idx_in = pltpu.make_async_copy(idx_hbm, idx_ref, small_sem.at[0])
    feat_in = []
    for num, (lo, hi) in enumerate(chunks):
        rows = pl.ds(lo, hi - lo)
        feat_in.append(pltpu.make_async_copy(feat_hbm.at[rows, :], feat_v.at[rows, :], feat_sem.at[num]))
    w0_in = pltpu.make_async_copy(w0_hbm, w0_ref, small_sem.at[1])
    w1_in = pltpu.make_async_copy(w1_hbm, w1_ref, small_sem.at[2])
    int_in = pltpu.make_async_copy(int_hbm, int_v, int_sem)
    halo_in = pltpu.make_async_copy(halo_hbm, halo_v, halo_sem)
    idx_in.start()
    feat_in[0].start()

    def pick_block(buf, start):
        node_ids = lax.broadcasted_iota(jnp.int16, (N_TILE, quarter), 0)
        plan = jnp.broadcast_to(idx_ref[buf:buf + 1, :] - start, (N_TILE, quarter)).astype(jnp.int16)
        return jnp.where(node_ids == plan, jnp.ones((), BF16), jnp.zeros((), BF16))

    def build_pick(*bufs):
        @pl.loop(0, nodes // N_TILE)
        def _(blk):
            start = pl.multiple_of(blk * N_TILE, N_TILE)
            for buf in bufs:
                pick_v[pl.ds(start, N_TILE), buf * quarter:(buf + 1) * quarter] = pick_block(buf, start)

    def remote(src, dst, send_sem, recv_sem, target):
        return pltpu.make_async_remote_copy(src_ref=src, dst_ref=dst, send_sem=send_sem, recv_sem=recv_sem, device_id=target, device_id_type=MESH)

    with jax.named_scope('idx_wait'):
        idx_in.wait()
    for copy in feat_in[1:]:
        copy.start()
    y_copies = []
    x_copies = []

    def send_y_rows(first, end):
        lo, hi = chunks[first][0], chunks[end - 1][1]
        rows = pl.ds(lo, hi - lo)
        with jax.named_scope(f'feat_wait{first}'):
            for copy in feat_in[first:end]:
                copy.wait()
        with jax.named_scope(f'gather_y{first}'):
            if first == 0:
                picked = None
                for start in range(0, nodes, N_TILE):
                    block = jnp.concatenate([pick_block(2, start), pick_block(3, start)], axis=1)
                    pick_v[start:start + N_TILE, half:] = block
                    part = dot(feat_v[rows, start:start + N_TILE], block, NN)
                    picked = part if picked is None else picked + part
                send_y[rows, :] = picked.astype(BF16)
            else:
                send_y[rows, :] = dot(feat_v[rows, :], pick_v[:, half:], NN).astype(BF16)
        if first == 0:
            with jax.named_scope('barrier'):
                pl.semaphore_wait(barrier, 3)
        for num in range(first, end):
            rows = pl.ds(chunks[num][0], chunks[num][1] - chunks[num][0])
            y_copies.append(remote(send_y.at[rows, :], recv_v.at[rows, half:], sy_sem.at[num], ry_sem.at[num], north))
            y_copies[-1].start()

    def send_x_rows(num):
        rows = pl.ds(x_parts[num][0], x_parts[num][1] - x_parts[num][0])
        with jax.named_scope(f'gather_x{num}'):
            picked = dot(feat_v[rows, :], pick_v[:, :half], NN).astype(BF16)
            send_x0[rows, :] = picked[:, :quarter]
            send_x1[rows, :] = picked[:, quarter:]
        x_copies.append(remote(send_x0.at[rows, :], recv_v.at[rows, :quarter], sx_sem.at[2 * num], rx_sem.at[2 * num], east))
        x_copies.append(remote(send_x1.at[rows, :], recv_v.at[rows, quarter:half], sx_sem.at[2 * num + 1], rx_sem.at[2 * num + 1], west))
        x_copies[-2].start()
        x_copies[-1].start()

    next_x = 0
    for first, end in [(0, 1), (1, 2), (2, 4), (4, len(chunks))]:
        send_y_rows(first, end)
        if first == 1:
            with jax.named_scope('pick_x'):
                build_pick(0, 1)
        if first == 0:
            for copy in (int_in, halo_in, w0_in, w1_in):
                copy.start()
        while next_x < len(x_parts) and x_parts[next_x][1] <= chunks[end - 1][1]:
            send_x_rows(next_x)
            next_x += 1

    with jax.named_scope('int_wait'):
        int_in.wait()
        halo_in.wait()
        w0_in.wait()
        w1_in.wait()
    with jax.named_scope('interior'):

        @pl.loop(0, nodes // BIG_COLS)
        def _(blk):
            cols = pl.ds(pl.multiple_of(blk * BIG_COLS, BIG_COLS), BIG_COLS)
            halo_t[:, cols] = halo_v[cols, :].T
            int_t[:, cols] = int_v[cols, :].T
            for lo, hi in big:
                z_int[lo:hi, cols] = dot(feat_v[lo:hi, :], int_v[cols, :], NT)

    def split3(value):
        high = value.astype(BF16)
        rest = value - high.astype(F32)
        middle = rest.astype(BF16)
        return high, middle, (rest - middle.astype(F32)).astype(BF16)

    last_lo, last_hi = chunks[-1]
    last = pl.ds(last_lo, last_hi - last_lo)
    tail = last_hi - last_lo
    with jax.named_scope('halo_pick'):
        halo_pick[...] = dot(halo_t[half:, :], pick_v[...], NN).astype(BF16)
    with jax.named_scope('xwait'):
        for copy in x_copies:
            copy.wait_recv()
    with jax.named_scope('last_x'):
        z_last = z_int[last, :] + dot(recv_v[last, :half], halo_t[:half, :], NN)
        z_int[last, :] = z_last
        for num, piece in enumerate(split3(z_last)):
            z_split[num * LAST_ROWS:num * LAST_ROWS + tail, :] = piece
    with jax.named_scope('last_pick'):
        parts = dot(z_split[...], pick_v[...], NN)
        z_pick[...] = parts[:LAST_ROWS] + parts[LAST_ROWS:2 * LAST_ROWS] + parts[2 * LAST_ROWS:]

    groups = [(0, 3)] + [(num, num + 1) for num in range(3, len(chunks) - 1)]
    for first, end in groups:
        lo, hi = chunks[first][0], chunks[end - 1][1]
        with jax.named_scope(f'ywait{first}'):
            for copy in y_copies[first:end]:
                copy.wait_recv()
        rows = pl.ds(lo, hi - lo)
        with jax.named_scope(f'yhalo{first}'):
            for col in range(0, nodes, HALO_COLS):
                cols = pl.ds(col, HALO_COLS)
                z_half[:hi - lo, cols] = (z_int[rows, cols] + dot(recv_v[rows, :], halo_t[:, cols], NN)).astype(BF16)
            part = dot(w0_ref[:, lo:hi], z_half[:hi - lo, :], NN)
            if first == 0:
                hid_acc[...] = part
            else:
                hid_acc[...] += part
    with jax.named_scope('hid_pick'):
        for num, piece in enumerate(split3(hid_acc[...])):
            hid_split[num * hid_rows:(num + 1) * hid_rows, :] = piece
        parts = dot(hid_split[...], pick_v[...], NN)
        hid_pick[...] = parts[:hid_rows] + parts[hid_rows:2 * hid_rows] + parts[2 * hid_rows:]

    second = [
        remote(send2_y, recv2_y, s2_sem.at[0], r2_sem.at[0], north),
        remote(send2_x0, recv2_x.at[:, :quarter], s2_sem.at[1], r2_sem.at[1], east),
        remote(send2_x1, recv2_x.at[:, quarter:], s2_sem.at[2], r2_sem.at[2], west),
    ]
    with jax.named_scope('ywait_last'):
        y_copies[-1].wait_recv()
    with jax.named_scope('sent2'):
        z_sent = (z_pick[:tail, :] + dot(recv_v[last, half:], halo_pick[...], NN)).astype(BF16)
        sent = hid_pick[...] + dot(w0_ref[:, last_lo:last_hi], z_sent, NN)
        sent = jnp.maximum(sent, 0.0).astype(BF16)
        send2_y[...] = sent[:, half:]
        send2_x0[...] = sent[:, :quarter]
        send2_x1[...] = sent[:, quarter:half]
    for copy in second:
        copy.start()
    with jax.named_scope('yhalo_last'):
        z_sum = (z_int[last, :] + dot(recv_v[last, half:], halo_t[half:, :], NN)).astype(BF16)
        hid_sum = hid_acc[...] + dot(w0_ref[:, last_lo:last_hi], z_sum, NN)
        hid_v[...] = jnp.maximum(hid_sum, 0.0).astype(BF16)
    with jax.named_scope('interior2'):
        hid_acc[...] = dot(hid_v[...], int_t[...], NN)
    with jax.named_scope('wait2x'):
        second[1].wait_recv()
        second[2].wait_recv()
    with jax.named_scope('xhalo2'):
        hid_acc[...] += dot(recv2_x[...], halo_t[:half, :], NN)
    with jax.named_scope('wait2y'):
        second[0].wait_recv()
    with jax.named_scope('yhalo2'):
        z_sum = hid_acc[...] + dot(recv2_y[...], halo_t[half:, :], NN)
        out_ref[...] = dot(w1_ref[...], z_sum.astype(BF16), NN).astype(BF16)
    with jax.named_scope('sendwait'):
        for copy in y_copies + x_copies + second:
            copy.wait_send()


def solution(mesh):
    grid_y = mesh.shape['tiley']
    grid_x = mesh.shape['tilex']
    node_spec = P(('parts', 'tiley', 'tilex'), None)
    full_spec = P(None, None)

    def per_device(node_feats, adj_int, adj_halo, send_idx, w_hidden, w_out):
        nodes, feat = node_feats.shape
        slots = adj_halo.shape[1]
        half, quarter = slots // 2, slots // 4
        hidden, classes = w_out.shape
        chunks = feature_chunks(feat)
        x_parts = x_chunks(feat)
        big = big_chunks(feat)
        vmem = pl.BlockSpec(memory_space=pltpu.VMEM)
        hbm = pl.BlockSpec(memory_space=pl.ANY)
        dma = pltpu.SemaphoreType.DMA
        out = pl.pallas_call(
            functools.partial(gcn_kernel, grid_y, grid_x, chunks, x_parts, big),
            out_shape=pltpu.VMEM((classes, nodes), BF16),
            in_specs=[hbm] * 6,
            out_specs=vmem,
            scratch_shapes=[
                pltpu.VMEM(send_idx.shape, jnp.int32),
                pltpu.VMEM((hidden, feat), BF16),
                pltpu.VMEM((classes, hidden), BF16),
                pltpu.VMEM((feat, nodes), BF16),
                pltpu.VMEM((nodes, nodes), BF16),
                pltpu.VMEM((nodes, nodes), BF16),
                pltpu.VMEM((nodes, slots), BF16),
                pltpu.VMEM((slots, nodes), BF16),
                pltpu.VMEM((nodes, slots), BF16),
                pltpu.VMEM((feat, half), BF16),
                pltpu.VMEM((feat, quarter), BF16),
                pltpu.VMEM((feat, quarter), BF16),
                pltpu.VMEM((feat, slots), BF16),
                pltpu.VMEM((feat, nodes), F32),
                pltpu.VMEM((512, nodes), BF16),
                pltpu.VMEM((half, slots), BF16),
                pltpu.VMEM((3 * LAST_ROWS, nodes), BF16),
                pltpu.VMEM((LAST_ROWS, slots), F32),
                pltpu.VMEM((3 * hidden, nodes), BF16),
                pltpu.VMEM((hidden, slots), F32),
                pltpu.VMEM((hidden, nodes), F32),
                pltpu.VMEM((hidden, nodes), BF16),
                pltpu.VMEM((hidden, half), BF16),
                pltpu.VMEM((hidden, quarter), BF16),
                pltpu.VMEM((hidden, quarter), BF16),
                pltpu.VMEM((hidden, half), BF16),
                pltpu.VMEM((hidden, half), BF16),
                dma((3,)),
                dma((len(chunks),)),
                dma,
                dma,
                dma((len(chunks),)),
                dma((len(chunks),)),
                dma((2 * len(x_parts),)),
                dma((2 * len(x_parts),)),
                dma((3,)),
                dma((3,)),
            ],
            compiler_params=pltpu.CompilerParams(collective_id=0, has_side_effects=True, vmem_limit_bytes=60 * 2**20),
        )(send_idx, w_hidden.T, w_out.T, node_feats.T, adj_int, adj_halo)
        return out.T

    return jax.shard_map(per_device, mesh=mesh, in_specs=(node_spec, node_spec, node_spec, node_spec, full_spec, full_spec), out_specs=node_spec, check_vma=False)
```

```python
import functools

import jax
import jax.numpy as jnp
from jax import lax
from jax.experimental import pallas as pl
from jax.experimental.pallas import tpu as pltpu
from jax.sharding import PartitionSpec as P

BF16 = jnp.bfloat16
F32 = jnp.float32
MESH = pl.DeviceIdType.MESH
N_TILE = 256
BIG_ROWS = 512
LAST_ROWS = 112
NUM_GATHERS = 4
BIG_COLS = 1024
HALO_COLS = 512
NN = (((1,), (0,)), ((), ()))
NT = (((1,), (1,)), ((), ()))


def dot(lhs, rhs, dims):
    return lax.dot_general(lhs, rhs, dims, preferred_element_type=F32)


def feature_chunks(feat):
    last = (feat - 96) // 16 * 16
    cuts = [0, 64, 256]
    while last - 128 - cuts[-1] > 256:
        cuts.append(cuts[-1] + 256)
    cuts += [last - 128, last, feat]
    return list(zip(cuts[:-1], cuts[1:]))


def big_chunks(feat):
    return [(lo, min(lo + BIG_ROWS, feat)) for lo in range(0, feat, BIG_ROWS)]


def x_chunks(feat):
    return [(0, BIG_ROWS), (BIG_ROWS, feat)]


def gcn_kernel(grid_y, grid_x, chunks, x_parts, big, idx_hbm, w0_hbm, w1_hbm, feat_hbm, int_hbm, halo_hbm, out_ref,
               idx_ref, w0_ref, w1_ref, feat_v, int_v, int_t, halo_v, halo_t, pick_v, send_y, send_x0, send_x1, recv_v, z_int, z_half, halo_pick, z_split, z_pick, hid_split, hid_pick, hid_acc,
               hid_v, send2_y, send2_x0, send2_x1, recv2_v,
               small_sem, feat_sem, int_sem, halo_sem, sy_sem, ry_sem, sx_sem, rx_sem, s2_sem, r2_sem, even_sem):
    me_y = lax.axis_index('tiley')
    me_x = lax.axis_index('tilex')
    east = {'tilex': lax.rem(me_x + 1, grid_x)}
    west = {'tilex': lax.rem(me_x + grid_x - 1, grid_x)}
    north = {'tiley': lax.rem(me_y + 1, grid_y)}
    nodes = int_v.shape[0]
    slots = halo_v.shape[1]
    half = slots // 2
    quarter = half // 2
    hid_rows = hid_v.shape[0]

    barrier = pltpu.get_barrier_semaphore()
    pl.semaphore_signal(barrier, inc=1, device_id=north, device_id_type=MESH)
    odd = lax.rem(me_x, 2)

    @pl.when(odd == 1)
    def _():
        for neighbour in (east, west):
            pl.semaphore_signal(barrier, inc=1, device_id=neighbour, device_id_type=MESH)

    idx_in = pltpu.make_async_copy(idx_hbm, idx_ref, small_sem.at[0])
    gathers = [(0, 1), (1, 2), (2, 4), (4, len(chunks))]
    feat_in = []
    for num, (first, end) in enumerate(gathers):
        rows = pl.ds(chunks[first][0], chunks[end - 1][1] - chunks[first][0])
        feat_in.append(pltpu.make_async_copy(feat_hbm.at[rows, :], feat_v.at[rows, :], feat_sem.at[num]))
    w0_in = pltpu.make_async_copy(w0_hbm, w0_ref, small_sem.at[1])
    w1_in = pltpu.make_async_copy(w1_hbm, w1_ref, small_sem.at[2])
    int_in = pltpu.make_async_copy(int_hbm, int_v, int_sem)
    halo_in = pltpu.make_async_copy(halo_hbm, halo_v, halo_sem)
    idx_in.start()
    feat_in[0].start()

    def pick_block(buf, start):
        node_ids = lax.broadcasted_iota(jnp.int16, (N_TILE, quarter), 0)
        plan = jnp.broadcast_to(idx_ref[buf:buf + 1, :] - start, (N_TILE, quarter)).astype(jnp.int16)
        return jnp.where(node_ids == plan, jnp.ones((), BF16), jnp.zeros((), BF16))

    def build_pick(*bufs):
        @pl.loop(0, nodes // N_TILE)
        def _(blk):
            start = pl.multiple_of(blk * N_TILE, N_TILE)
            for buf in bufs:
                pick_v[pl.ds(start, N_TILE), buf * quarter:(buf + 1) * quarter] = pick_block(buf, start)

    def remote(src, dst, send_sem, recv_sem, target):
        return pltpu.make_async_remote_copy(src_ref=src, dst_ref=dst, send_sem=send_sem, recv_sem=recv_sem, device_id=target, device_id_type=MESH)

    with jax.named_scope('idx_wait'):
        idx_in.wait()
    for copy in feat_in[1:]:
        copy.start()
    y_copies = []
    x_copies = []

    def first_piece(rows):
        picked = None
        for start in range(0, nodes, N_TILE):
            block = jnp.concatenate([pick_block(2, start), pick_block(3, start)], axis=1)
            pick_v[start:start + N_TILE, half:] = block
            part = dot(feat_v[rows, start:start + N_TILE], block, NN)
            picked = part if picked is None else picked + part
        send_y[rows, :] = picked.astype(BF16)

    def send_y_rows(num, first, end):
        lo, hi = chunks[first][0], chunks[end - 1][1]
        rows = pl.ds(lo, hi - lo)
        with jax.named_scope(f'feat_wait{first}'):
            feat_in[num].wait()
        with jax.named_scope(f'gather_y{first}'):
            if first > 0:
                send_y[rows, :] = dot(feat_v[rows, :], pick_v[:, half:], NN).astype(BF16)
            else:
                first_piece(rows)
        if first == 0:
            with jax.named_scope('barrier'):
                pl.semaphore_wait(barrier, 3 - 2 * odd)

                @pl.when(odd == 0)
                def _():
                    for neighbour in (east, west):
                        pl.semaphore_signal(even_sem, inc=1, device_id=neighbour, device_id_type=MESH)

        for chunk in range(first, end):
            rows = pl.ds(chunks[chunk][0], chunks[chunk][1] - chunks[chunk][0])
            y_copies.append(remote(send_y.at[rows, :], recv_v.at[rows, half:], sy_sem, ry_sem.at[chunk], north))
            y_copies[-1].start()

    def send_x_rows(num):
        rows = pl.ds(x_parts[num][0], x_parts[num][1] - x_parts[num][0])
        with jax.named_scope(f'gather_x{num}'):
            picked = dot(feat_v[rows, :], pick_v[:, :half], NN).astype(BF16)
            send_x0[rows, :] = picked[:, :quarter]
            send_x1[rows, :] = picked[:, quarter:]
        if num == 0:

            @pl.when(odd == 1)
            def _():
                pl.semaphore_wait(even_sem, 2)

        x_copies.append(remote(send_x0.at[rows, :], recv_v.at[rows, :quarter], sx_sem.at[0], rx_sem.at[0], east))
        x_copies.append(remote(send_x1.at[rows, :], recv_v.at[rows, quarter:half], sx_sem.at[1], rx_sem.at[1], west))
        x_copies[-2].start()
        x_copies[-1].start()

    next_x = 0
    for num, (first, end) in enumerate(gathers):
        send_y_rows(num, first, end)
        if first == 1:
            with jax.named_scope('pick_x'):
                build_pick(0, 1)
        if first == 0:
            for copy in (int_in, halo_in, w0_in, w1_in):
                copy.start()
        while next_x < len(x_parts) and x_parts[next_x][1] <= chunks[end - 1][1]:
            send_x_rows(next_x)
            next_x += 1

    with jax.named_scope('int_wait'):
        int_in.wait()
        halo_in.wait()
        w0_in.wait()
        w1_in.wait()
    with jax.named_scope('interior'):

        @pl.loop(0, nodes // BIG_COLS)
        def _(blk):
            cols = pl.ds(pl.multiple_of(blk * BIG_COLS, BIG_COLS), BIG_COLS)
            halo_t[:, cols] = halo_v[cols, :].T
            int_t[:, cols] = int_v[cols, :].T
            for lo, hi in big:
                z_int[lo:hi, cols] = dot(feat_v[lo:hi, :], int_v[cols, :], NT)

    def split3(value):
        high = value.astype(BF16)
        rest = value - high.astype(F32)
        middle = rest.astype(BF16)
        return high, middle, (rest - middle.astype(F32)).astype(BF16)

    last_lo, last_hi = chunks[-1]
    last = pl.ds(last_lo, last_hi - last_lo)
    tail = last_hi - last_lo
    with jax.named_scope('halo_pick'):
        halo_pick[...] = dot(halo_t[half:, :], pick_v[...], NN).astype(BF16)
    with jax.named_scope('xwait'):
        x_whole = [
            remote(send_x0, recv_v.at[:, :quarter], sx_sem.at[0], rx_sem.at[0], east),
            remote(send_x1, recv_v.at[:, quarter:half], sx_sem.at[1], rx_sem.at[1], west),
        ]
        for copy in x_whole:
            copy.wait_recv()
    with jax.named_scope('last_x'):
        z_last = z_int[last, :] + dot(recv_v[last, :half], halo_t[:half, :], NN)
        z_int[last, :] = z_last
        for num, piece in enumerate(split3(z_last)):
            z_split[num * LAST_ROWS:num * LAST_ROWS + tail, :] = piece
    with jax.named_scope('last_pick'):
        parts = dot(z_split[...], pick_v[...], NN)
        z_pick[...] = parts[:LAST_ROWS] + parts[LAST_ROWS:2 * LAST_ROWS] + parts[2 * LAST_ROWS:]

    groups = [(0, 3)] + [(num, num + 1) for num in range(3, len(chunks) - 1)]
    for first, end in groups:
        lo, hi = chunks[first][0], chunks[end - 1][1]
        with jax.named_scope(f'ywait{first}'):
            for copy in y_copies[first:end]:
                copy.wait_recv()
        rows = pl.ds(lo, hi - lo)
        with jax.named_scope(f'yhalo{first}'):
            for col in range(0, nodes, HALO_COLS):
                cols = pl.ds(col, HALO_COLS)
                z_half[:hi - lo, cols] = (z_int[rows, cols] + dot(recv_v[rows, :], halo_t[:, cols], NN)).astype(BF16)
            part = dot(w0_ref[:, lo:hi], z_half[:hi - lo, :], NN)
            if first == 0:
                hid_acc[...] = part
            else:
                hid_acc[...] += part
    with jax.named_scope('hid_pick'):
        for num, piece in enumerate(split3(hid_acc[...])):
            hid_split[num * hid_rows:(num + 1) * hid_rows, :] = piece
        parts = dot(hid_split[...], pick_v[...], NN)
        hid_pick[...] = parts[:hid_rows] + parts[hid_rows:2 * hid_rows] + parts[2 * hid_rows:]

    second = [
        remote(send2_y, recv2_v.at[:, half:], s2_sem.at[0], r2_sem.at[0], north),
        remote(send2_x0, recv2_v.at[:, :quarter], s2_sem.at[1], r2_sem.at[1], east),
        remote(send2_x1, recv2_v.at[:, quarter:half], s2_sem.at[2], r2_sem.at[2], west),
    ]
    with jax.named_scope('ywait_last'):
        y_copies[-1].wait_recv()
    with jax.named_scope('sent2'):
        z_sent = (z_pick[:tail, :] + dot(recv_v[last, half:], halo_pick[...], NN)).astype(BF16)
        sent = hid_pick[...] + dot(w0_ref[:, last_lo:last_hi], z_sent, NN)
        sent = jnp.maximum(sent, 0.0).astype(BF16)
        send2_y[...] = sent[:, half:]
        send2_x0[...] = sent[:, :quarter]
        send2_x1[...] = sent[:, quarter:half]
    for copy in second:
        copy.start()
    with jax.named_scope('yhalo_last'):
        z_sum = (z_int[last, :] + dot(recv_v[last, half:], halo_t[half:, :], NN)).astype(BF16)
        hid_sum = hid_acc[...] + dot(w0_ref[:, last_lo:last_hi], z_sum, NN)
        hid_v[...] = jnp.maximum(hid_sum, 0.0).astype(BF16)
    with jax.named_scope('interior2'):
        hid_acc[...] = dot(hid_v[...], int_t[...], NN)
    from_y, from_west, from_east = second

    def halo_part(lo, hi):
        return dot(recv2_v[:, lo:hi], halo_t[lo:hi, :], NN)

    def finish(parts):
        z_sum = hid_acc[...]
        for copies, lo, hi in parts:
            for copy in copies:
                copy.wait_recv()
            z_sum = z_sum + halo_part(lo, hi)
        out_ref[...] = dot(w1_ref[...], z_sum.astype(BF16), NN).astype(BF16)

    with jax.named_scope('halo2'):

        @pl.when(odd == 1)
        def _():
            finish([([from_y], half, slots), ([from_west, from_east], 0, half)])

        @pl.when(odd == 0)
        def _():
            finish([([from_west, from_east], 0, half), ([from_y], half, slots)])

    with jax.named_scope('sendwait'):
        for copy in [remote(send_y, recv_v.at[:, half:], sy_sem, ry_sem.at[0], north)] + x_whole + second:
            copy.wait_send()


def solution(mesh):
    grid_y = mesh.shape['tiley']
    grid_x = mesh.shape['tilex']
    node_spec = P(('parts', 'tiley', 'tilex'), None)
    full_spec = P(None, None)

    def per_device(node_feats, adj_int, adj_halo, send_idx, w_hidden, w_out):
        nodes, feat = node_feats.shape
        slots = adj_halo.shape[1]
        half, quarter = slots // 2, slots // 4
        hidden, classes = w_out.shape
        chunks = feature_chunks(feat)
        x_parts = x_chunks(feat)
        big = big_chunks(feat)
        vmem = pl.BlockSpec(memory_space=pltpu.VMEM)
        hbm = pl.BlockSpec(memory_space=pl.ANY)
        dma = pltpu.SemaphoreType.DMA
        out = pl.pallas_call(
            functools.partial(gcn_kernel, grid_y, grid_x, chunks, x_parts, big),
            out_shape=pltpu.VMEM((classes, nodes), BF16),
            in_specs=[hbm] * 6,
            out_specs=vmem,
            scratch_shapes=[
                pltpu.VMEM(send_idx.shape, jnp.int32),
                pltpu.VMEM((hidden, feat), BF16),
                pltpu.VMEM((classes, hidden), BF16),
                pltpu.VMEM((feat, nodes), BF16),
                pltpu.VMEM((nodes, nodes), BF16),
                pltpu.VMEM((nodes, nodes), BF16),
                pltpu.VMEM((nodes, slots), BF16),
                pltpu.VMEM((slots, nodes), BF16),
                pltpu.VMEM((nodes, slots), BF16),
                pltpu.VMEM((feat, half), BF16),
                pltpu.VMEM((feat, quarter), BF16),
                pltpu.VMEM((feat, quarter), BF16),
                pltpu.VMEM((feat, slots), BF16),
                pltpu.VMEM((feat, nodes), F32),
                pltpu.VMEM((512, nodes), BF16),
                pltpu.VMEM((half, slots), BF16),
                pltpu.VMEM((3 * LAST_ROWS, nodes), BF16),
                pltpu.VMEM((LAST_ROWS, slots), F32),
                pltpu.VMEM((3 * hidden, nodes), BF16),
                pltpu.VMEM((hidden, slots), F32),
                pltpu.VMEM((hidden, nodes), F32),
                pltpu.VMEM((hidden, nodes), BF16),
                pltpu.VMEM((hidden, half), BF16),
                pltpu.VMEM((hidden, quarter), BF16),
                pltpu.VMEM((hidden, quarter), BF16),
                pltpu.VMEM((hidden, slots), BF16),
                dma((3,)),
                dma((NUM_GATHERS,)),
                dma,
                dma,
                dma,
                dma((len(chunks),)),
                dma((2,)),
                dma((2,)),
                dma((3,)),
                dma((3,)),
                pltpu.SemaphoreType.REGULAR,
            ],
            compiler_params=pltpu.CompilerParams(collective_id=0, has_side_effects=True, vmem_limit_bytes=60 * 2**20),
        )(send_idx, w_hidden.T, w_out.T, node_feats.T, adj_int, adj_halo)
        return out.T

    return jax.shard_map(per_device, mesh=mesh, in_specs=(node_spec, node_spec, node_spec, node_spec, full_spec, full_spec), out_specs=node_spec, check_vma=False)
```

```python
import functools

import jax
import jax.numpy as jnp
from jax import lax
from jax.experimental import pallas as pl
from jax.experimental.pallas import tpu as pltpu
from jax.sharding import PartitionSpec as P

BF16 = jnp.bfloat16
F32 = jnp.float32
MESH = pl.DeviceIdType.MESH
N_TILE = 256
BIG_ROWS = 512
LAST_ROWS = 112
NUM_GATHERS = 4
BIG_COLS = 2048
HALO_COLS = 512
NN = (((1,), (0,)), ((), ()))
NT = (((1,), (1,)), ((), ()))


def dot(lhs, rhs, dims):
    return lax.dot_general(lhs, rhs, dims, preferred_element_type=F32)


def feature_chunks(feat):
    last = (feat - 96) // 16 * 16
    cuts = [0, 64, 256]
    while last - 128 - cuts[-1] > 256:
        cuts.append(cuts[-1] + 256)
    cuts += [last - 128, last, feat]
    return list(zip(cuts[:-1], cuts[1:]))


def big_chunks(feat):
    return [(lo, min(lo + BIG_ROWS, feat)) for lo in range(0, feat, BIG_ROWS)]


def x_chunks(feat):
    return [(0, BIG_ROWS), (BIG_ROWS, feat)]


def gcn_kernel(grid_y, grid_x, chunks, x_parts, big, idx_hbm, w0_hbm, w1_hbm, feat_hbm, int_hbm, halo_hbm, out_ref,
               idx_ref, w0_ref, w1_ref, feat_v, int_v, int_t, halo_v, halo_t, pick_v, send_y, send_x0, send_x1, recv_v, z_int, z_half, halo_pick, z_split, z_pick, hid_split, hid_pick, hid_acc,
               hid_v, send2_y, send2_x0, send2_x1, recv2_v,
               small_sem, feat_sem, int_sem, halo_sem, sy_sem, ry_sem, sx_sem, rx_sem, s2_sem, r2_sem, even_sem):
    me_y = lax.axis_index('tiley')
    me_x = lax.axis_index('tilex')
    east = {'tilex': lax.rem(me_x + 1, grid_x)}
    west = {'tilex': lax.rem(me_x + grid_x - 1, grid_x)}
    north = {'tiley': lax.rem(me_y + 1, grid_y)}
    nodes = int_v.shape[0]
    slots = halo_v.shape[1]
    half = slots // 2
    quarter = half // 2
    hid_rows = hid_v.shape[0]

    barrier = pltpu.get_barrier_semaphore()
    pl.semaphore_signal(barrier, inc=1, device_id=north, device_id_type=MESH)
    odd = lax.rem(me_x, 2)

    @pl.when(odd == 1)
    def _():
        for neighbour in (east, west):
            pl.semaphore_signal(barrier, inc=1, device_id=neighbour, device_id_type=MESH)

    idx_in = pltpu.make_async_copy(idx_hbm, idx_ref, small_sem.at[0])
    gathers = [(0, 1), (1, 2), (2, 4), (4, len(chunks))]
    feat_in = []
    for num, (first, end) in enumerate(gathers):
        rows = pl.ds(chunks[first][0], chunks[end - 1][1] - chunks[first][0])
        feat_in.append(pltpu.make_async_copy(feat_hbm.at[rows, :], feat_v.at[rows, :], feat_sem.at[num]))
    w0_in = pltpu.make_async_copy(w0_hbm, w0_ref, small_sem.at[1])
    w1_in = pltpu.make_async_copy(w1_hbm, w1_ref, small_sem.at[2])
    int_in = pltpu.make_async_copy(int_hbm, int_v, int_sem)
    halo_in = pltpu.make_async_copy(halo_hbm, halo_v, halo_sem)
    idx_in.start()
    feat_in[0].start()

    def pick_block(buf, start):
        node_ids = lax.broadcasted_iota(jnp.int16, (N_TILE, quarter), 0)
        plan = jnp.broadcast_to(idx_ref[buf:buf + 1, :] - start, (N_TILE, quarter)).astype(jnp.int16)
        return jnp.where(node_ids == plan, jnp.ones((), BF16), jnp.zeros((), BF16))

    def build_pick(*bufs):
        @pl.loop(0, nodes // N_TILE)
        def _(blk):
            start = pl.multiple_of(blk * N_TILE, N_TILE)
            for buf in bufs:
                pick_v[pl.ds(start, N_TILE), buf * quarter:(buf + 1) * quarter] = pick_block(buf, start)

    def remote(src, dst, send_sem, recv_sem, target):
        return pltpu.make_async_remote_copy(src_ref=src, dst_ref=dst, send_sem=send_sem, recv_sem=recv_sem, device_id=target, device_id_type=MESH)

    with jax.named_scope('idx_wait'):
        idx_in.wait()
    for copy in feat_in[1:]:
        copy.start()
    y_copies = []
    x_copies = []

    def first_piece(rows):
        picked = None
        for start in range(0, nodes, N_TILE):
            block = jnp.concatenate([pick_block(2, start), pick_block(3, start)], axis=1)
            pick_v[start:start + N_TILE, half:] = block
            part = dot(feat_v[rows, start:start + N_TILE], block, NN)
            picked = part if picked is None else picked + part
        send_y[rows, :] = picked.astype(BF16)

    def send_y_rows(num, first, end):
        lo, hi = chunks[first][0], chunks[end - 1][1]
        rows = pl.ds(lo, hi - lo)
        with jax.named_scope(f'feat_wait{first}'):
            feat_in[num].wait()
        with jax.named_scope(f'gather_y{first}'):
            if first > 0:
                send_y[rows, :] = dot(feat_v[rows, :], pick_v[:, half:], NN).astype(BF16)
            else:
                first_piece(rows)
        if first == 0:
            with jax.named_scope('barrier'):
                pl.semaphore_wait(barrier, 3 - 2 * odd)

                @pl.when(odd == 0)
                def _():
                    for neighbour in (east, west):
                        pl.semaphore_signal(even_sem, inc=1, device_id=neighbour, device_id_type=MESH)

        for chunk in range(first, end):
            rows = pl.ds(chunks[chunk][0], chunks[chunk][1] - chunks[chunk][0])
            y_copies.append(remote(send_y.at[rows, :], recv_v.at[rows, half:], sy_sem, ry_sem.at[chunk], north))
            y_copies[-1].start()

    def send_x_rows(num):
        rows = pl.ds(x_parts[num][0], x_parts[num][1] - x_parts[num][0])
        with jax.named_scope(f'gather_x{num}'):
            picked = dot(feat_v[rows, :], pick_v[:, :half], NN).astype(BF16)
            send_x0[rows, :] = picked[:, :quarter]
            send_x1[rows, :] = picked[:, quarter:]
        if num == 0:

            @pl.when(odd == 1)
            def _():
                pl.semaphore_wait(even_sem, 2)

        x_copies.append(remote(send_x0.at[rows, :], recv_v.at[rows, :quarter], sx_sem.at[0], rx_sem.at[0], east))
        x_copies.append(remote(send_x1.at[rows, :], recv_v.at[rows, quarter:half], sx_sem.at[1], rx_sem.at[1], west))
        x_copies[-2].start()
        x_copies[-1].start()

    next_x = 0
    for num, (first, end) in enumerate(gathers):
        send_y_rows(num, first, end)
        if first == 1:
            with jax.named_scope('pick_x'):
                build_pick(0, 1)
        if first == 0:
            for copy in (int_in, halo_in, w0_in, w1_in):
                copy.start()
        while next_x < len(x_parts) and x_parts[next_x][1] <= chunks[end - 1][1]:
            send_x_rows(next_x)
            next_x += 1

    with jax.named_scope('int_wait'):
        int_in.wait()
        halo_in.wait()
        w0_in.wait()
        w1_in.wait()
    with jax.named_scope('interior'):

        @pl.loop(0, nodes // BIG_COLS)
        def _(blk):
            cols = pl.ds(pl.multiple_of(blk * BIG_COLS, BIG_COLS), BIG_COLS)
            halo_t[:, cols] = halo_v[cols, :].T
            int_t[:, cols] = int_v[cols, :].T
            for lo, hi in big:
                z_int[lo:hi, cols] = dot(feat_v[lo:hi, :], int_v[cols, :], NT)

    def split3(value):
        high = value.astype(BF16)
        rest = value - high.astype(F32)
        middle = rest.astype(BF16)
        return high, middle, (rest - middle.astype(F32)).astype(BF16)

    last_lo, last_hi = chunks[-1]
    last = pl.ds(last_lo, last_hi - last_lo)
    tail = last_hi - last_lo
    with jax.named_scope('halo_pick'):
        halo_pick[...] = dot(halo_t[half:, :], pick_v[...], NN).astype(BF16)
    with jax.named_scope('xwait'):
        x_whole = [
            remote(send_x0, recv_v.at[:, :quarter], sx_sem.at[0], rx_sem.at[0], east),
            remote(send_x1, recv_v.at[:, quarter:half], sx_sem.at[1], rx_sem.at[1], west),
        ]
        for copy in x_whole:
            copy.wait_recv()
    with jax.named_scope('last_x'):
        z_last = z_int[last, :] + dot(recv_v[last, :half], halo_t[:half, :], NN)
        z_int[last, :] = z_last
        for num, piece in enumerate(split3(z_last)):
            z_split[num * LAST_ROWS:num * LAST_ROWS + tail, :] = piece
    with jax.named_scope('last_pick'):
        parts = dot(z_split[...], pick_v[...], NN)
        z_pick[...] = parts[:LAST_ROWS] + parts[LAST_ROWS:2 * LAST_ROWS] + parts[2 * LAST_ROWS:]

    groups = [(0, 3)] + [(num, num + 1) for num in range(3, len(chunks) - 1)]
    for first, end in groups:
        lo, hi = chunks[first][0], chunks[end - 1][1]
        with jax.named_scope(f'ywait{first}'):
            for copy in y_copies[first:end]:
                copy.wait_recv()
        rows = pl.ds(lo, hi - lo)
        with jax.named_scope(f'yhalo{first}'):
            for col in range(0, nodes, HALO_COLS):
                cols = pl.ds(col, HALO_COLS)
                z_half[:hi - lo, cols] = (z_int[rows, cols] + dot(recv_v[rows, :], halo_t[:, cols], NN)).astype(BF16)
            part = dot(w0_ref[:, lo:hi], z_half[:hi - lo, :], NN)
            if first == 0:
                hid_acc[...] = part
            else:
                hid_acc[...] += part
    with jax.named_scope('hid_pick'):
        for num, piece in enumerate(split3(hid_acc[...])):
            hid_split[num * hid_rows:(num + 1) * hid_rows, :] = piece
        parts = dot(hid_split[...], pick_v[...], NN)
        hid_pick[...] = parts[:hid_rows] + parts[hid_rows:2 * hid_rows] + parts[2 * hid_rows:]

    second = [
        remote(send2_y, recv2_v.at[:, half:], s2_sem.at[0], r2_sem.at[0], north),
        remote(send2_x0, recv2_v.at[:, :quarter], s2_sem.at[1], r2_sem.at[1], east),
        remote(send2_x1, recv2_v.at[:, quarter:half], s2_sem.at[2], r2_sem.at[2], west),
    ]
    with jax.named_scope('ywait_last'):
        y_copies[-1].wait_recv()
    with jax.named_scope('sent2'):
        z_sent = (z_pick[:tail, :] + dot(recv_v[last, half:], halo_pick[...], NN)).astype(BF16)
        sent = hid_pick[...] + dot(w0_ref[:, last_lo:last_hi], z_sent, NN)
        sent = jnp.maximum(sent, 0.0).astype(BF16)
        send2_y[...] = sent[:, half:]
        send2_x0[...] = sent[:, :quarter]
        send2_x1[...] = sent[:, quarter:half]
    for copy in second:
        copy.start()
    with jax.named_scope('yhalo_last'):
        z_sum = (z_int[last, :] + dot(recv_v[last, half:], halo_t[half:, :], NN)).astype(BF16)
        hid_sum = hid_acc[...] + dot(w0_ref[:, last_lo:last_hi], z_sum, NN)
        hid_v[...] = jnp.maximum(hid_sum, 0.0).astype(BF16)
    with jax.named_scope('interior2'):
        hid_acc[...] = dot(hid_v[...], int_t[...], NN)
    from_y, from_west, from_east = second

    def halo_part(lo, hi):
        return dot(recv2_v[:, lo:hi], halo_t[lo:hi, :], NN)

    def finish(parts):
        z_sum = hid_acc[...]
        for num, (copies, lo, hi) in enumerate(parts):
            with jax.named_scope(f'finwait{num}'):
                for copy in copies:
                    copy.wait_recv()
            z_sum = z_sum + halo_part(lo, hi)
        out_ref[...] = dot(w1_ref[...], z_sum.astype(BF16), NN).astype(BF16)

    with jax.named_scope('halo2'):

        @pl.when(odd == 1)
        def _():
            finish([([from_y], half, slots), ([from_west], 0, quarter), ([from_east], quarter, half)])

        @pl.when(odd == 0)
        def _():
            finish([([from_east], quarter, half), ([from_west], 0, quarter), ([from_y], half, slots)])

    with jax.named_scope('sendwait'):
        for copy in [remote(send_y, recv_v.at[:, half:], sy_sem, ry_sem.at[0], north)] + x_whole + second:
            copy.wait_send()


def solution(mesh):
    grid_y = mesh.shape['tiley']
    grid_x = mesh.shape['tilex']
    node_spec = P(('parts', 'tiley', 'tilex'), None)
    full_spec = P(None, None)

    def per_device(node_feats, adj_int, adj_halo, send_idx, w_hidden, w_out):
        nodes, feat = node_feats.shape
        slots = adj_halo.shape[1]
        half, quarter = slots // 2, slots // 4
        hidden, classes = w_out.shape
        chunks = feature_chunks(feat)
        x_parts = x_chunks(feat)
        big = big_chunks(feat)
        vmem = pl.BlockSpec(memory_space=pltpu.VMEM)
        hbm = pl.BlockSpec(memory_space=pl.ANY)
        dma = pltpu.SemaphoreType.DMA
        out = pl.pallas_call(
            functools.partial(gcn_kernel, grid_y, grid_x, chunks, x_parts, big),
            out_shape=pltpu.VMEM((classes, nodes), BF16),
            in_specs=[hbm] * 6,
            out_specs=vmem,
            scratch_shapes=[
                pltpu.VMEM(send_idx.shape, jnp.int32),
                pltpu.VMEM((hidden, feat), BF16),
                pltpu.VMEM((classes, hidden), BF16),
                pltpu.VMEM((feat, nodes), BF16),
                pltpu.VMEM((nodes, nodes), BF16),
                pltpu.VMEM((nodes, nodes), BF16),
                pltpu.VMEM((nodes, slots), BF16),
                pltpu.VMEM((slots, nodes), BF16),
                pltpu.VMEM((nodes, slots), BF16),
                pltpu.VMEM((feat, half), BF16),
                pltpu.VMEM((feat, quarter), BF16),
                pltpu.VMEM((feat, quarter), BF16),
                pltpu.VMEM((feat, slots), BF16),
                pltpu.VMEM((feat, nodes), F32),
                pltpu.VMEM((512, nodes), BF16),
                pltpu.VMEM((half, slots), BF16),
                pltpu.VMEM((3 * LAST_ROWS, nodes), BF16),
                pltpu.VMEM((LAST_ROWS, slots), F32),
                pltpu.VMEM((3 * hidden, nodes), BF16),
                pltpu.VMEM((hidden, slots), F32),
                pltpu.VMEM((hidden, nodes), F32),
                pltpu.VMEM((hidden, nodes), BF16),
                pltpu.VMEM((hidden, half), BF16),
                pltpu.VMEM((hidden, quarter), BF16),
                pltpu.VMEM((hidden, quarter), BF16),
                pltpu.VMEM((hidden, slots), BF16),
                dma((3,)),
                dma((NUM_GATHERS,)),
                dma,
                dma,
                dma,
                dma((len(chunks),)),
                dma((2,)),
                dma((2,)),
                dma((3,)),
                dma((3,)),
                pltpu.SemaphoreType.REGULAR,
            ],
            compiler_params=pltpu.CompilerParams(collective_id=0, has_side_effects=True, vmem_limit_bytes=60 * 2**20),
        )(send_idx, w_hidden.T, w_out.T, node_feats.T, adj_int, adj_halo)
        return out.T

    return jax.shard_map(per_device, mesh=mesh, in_specs=(node_spec, node_spec, node_spec, node_spec, full_spec, full_spec), out_specs=node_spec, check_vma=False)
```

```python
import functools

import jax
import jax.numpy as jnp
from jax import lax
from jax.experimental import pallas as pl
from jax.experimental.pallas import tpu as pltpu
from jax.sharding import PartitionSpec as P

BF16 = jnp.bfloat16
F32 = jnp.float32
MESH = pl.DeviceIdType.MESH
N_TILE = 256
BIG_ROWS = 512
LAST_ROWS = 112
NUM_GATHERS = 4
BIG_COLS = 2048
HALO_COLS = 512
NN = (((1,), (0,)), ((), ()))
NT = (((1,), (1,)), ((), ()))


def dot(lhs, rhs, dims):
    return lax.dot_general(lhs, rhs, dims, preferred_element_type=F32)


def feature_chunks(feat):
    last = (feat - 96) // 16 * 16
    cuts = [0, 64, 256]
    while last - 128 - cuts[-1] > 256:
        cuts.append(cuts[-1] + 256)
    cuts += [last - 128, last, feat]
    return list(zip(cuts[:-1], cuts[1:]))


def big_chunks(feat):
    return [(lo, min(lo + BIG_ROWS, feat)) for lo in range(0, feat, BIG_ROWS)]


def x_chunks(feat):
    return [(0, BIG_ROWS), (BIG_ROWS, feat)]


def gcn_kernel(grid_y, grid_x, chunks, x_parts, big, idx_hbm, w0_hbm, w1_hbm, feat_hbm, int_hbm, halo_hbm, out_ref,
               idx_ref, w0_ref, w1_ref, feat_v, int_v, int_t, halo_v, halo_t, pick_v, send_y, send_x, recv_v, z_int, z_half, halo_pick, z_split, z_pick, hid_split, hid_pick, hid_acc,
               hid_v, send2_v, recv2_v,
               small_sem, feat_sem, int_sem, halo_sem, sy_sem, ry_sem, sx_sem, rx_sem, s2_sem, r2_sem, even_sem):
    me_y = lax.axis_index('tiley')
    me_x = lax.axis_index('tilex')
    east = {'tilex': lax.rem(me_x + 1, grid_x)}
    west = {'tilex': lax.rem(me_x + grid_x - 1, grid_x)}
    north = {'tiley': lax.rem(me_y + 1, grid_y)}
    nodes = int_v.shape[0]
    slots = halo_v.shape[1]
    half = slots // 2
    quarter = half // 2
    hid_rows = hid_v.shape[0]

    barrier = pltpu.get_barrier_semaphore()
    pl.semaphore_signal(barrier, inc=1, device_id=north, device_id_type=MESH)
    odd = lax.rem(me_x, 2)

    @pl.when(odd == 1)
    def _():
        for neighbour in (east, west):
            pl.semaphore_signal(barrier, inc=1, device_id=neighbour, device_id_type=MESH)

    idx_in = pltpu.make_async_copy(idx_hbm, idx_ref, small_sem.at[0])
    gathers = [(0, 1), (1, 2), (2, 4), (4, len(chunks))]
    feat_in = []
    for num, (first, end) in enumerate(gathers):
        rows = pl.ds(chunks[first][0], chunks[end - 1][1] - chunks[first][0])
        feat_in.append(pltpu.make_async_copy(feat_hbm.at[rows, :], feat_v.at[rows, :], feat_sem.at[num]))
    w0_in = pltpu.make_async_copy(w0_hbm, w0_ref, small_sem.at[1])
    w1_in = pltpu.make_async_copy(w1_hbm, w1_ref, small_sem.at[2])
    int_in = pltpu.make_async_copy(int_hbm, int_v, int_sem)
    halo_in = pltpu.make_async_copy(halo_hbm, halo_v, halo_sem)
    idx_in.start()
    feat_in[0].start()

    def pick_block(buf, start):
        node_ids = lax.broadcasted_iota(jnp.int16, (N_TILE, quarter), 0)
        plan = jnp.broadcast_to(idx_ref[buf:buf + 1, :] - start, (N_TILE, quarter)).astype(jnp.int16)
        return jnp.where(node_ids == plan, jnp.ones((), BF16), jnp.zeros((), BF16))

    def build_pick(*bufs):
        @pl.loop(0, nodes // N_TILE)
        def _(blk):
            start = pl.multiple_of(blk * N_TILE, N_TILE)
            for buf in bufs:
                pick_v[pl.ds(start, N_TILE), buf * quarter:(buf + 1) * quarter] = pick_block(buf, start)

    def remote(src, dst, send_sem, recv_sem, target):
        return pltpu.make_async_remote_copy(src_ref=src, dst_ref=dst, send_sem=send_sem, recv_sem=recv_sem, device_id=target, device_id_type=MESH)

    with jax.named_scope('idx_wait'):
        idx_in.wait()
    for copy in feat_in[1:]:
        copy.start()
    y_copies = []
    x_copies = []

    def first_piece(rows):
        picked = None
        for start in range(0, nodes, N_TILE):
            block = jnp.concatenate([pick_block(2, start), pick_block(3, start)], axis=1)
            pick_v[start:start + N_TILE, half:] = block
            part = dot(feat_v[rows, start:start + N_TILE], block, NN)
            picked = part if picked is None else picked + part
        send_y[rows, :] = picked.astype(BF16)

    def send_y_rows(num, first, end):
        lo, hi = chunks[first][0], chunks[end - 1][1]
        rows = pl.ds(lo, hi - lo)
        with jax.named_scope(f'feat_wait{first}'):
            feat_in[num].wait()
        with jax.named_scope(f'gather_y{first}'):
            if first > 0:
                send_y[rows, :] = dot(feat_v[rows, :], pick_v[:, half:], NN).astype(BF16)
            else:
                first_piece(rows)
        if first == 0:
            with jax.named_scope('barrier'):
                pl.semaphore_wait(barrier, 3 - 2 * odd)

                @pl.when(odd == 0)
                def _():
                    for neighbour in (east, west):
                        pl.semaphore_signal(even_sem, inc=1, device_id=neighbour, device_id_type=MESH)

        for chunk in range(first, end):
            rows = pl.ds(chunks[chunk][0], chunks[chunk][1] - chunks[chunk][0])
            y_copies.append(remote(send_y.at[rows, :], recv_v.at[rows, half:], sy_sem, ry_sem.at[max(chunk - 2, 0)], north))
            y_copies[-1].start()

    def send_x_rows(num):
        rows = pl.ds(x_parts[num][0], x_parts[num][1] - x_parts[num][0])
        with jax.named_scope(f'gather_x{num}'):
            picked = dot(feat_v[rows, :], pick_v[:, :half], NN).astype(BF16)
            send_x[rows, :] = picked
        if num == 0:

            @pl.when(odd == 1)
            def _():
                pl.semaphore_wait(even_sem, 2)

        x_copies.append(remote(send_x.at[rows, :quarter], recv_v.at[rows, :quarter], sx_sem, rx_sem, east))
        x_copies.append(remote(send_x.at[rows, quarter:], recv_v.at[rows, quarter:half], sx_sem, rx_sem, west))
        x_copies[-2].start()
        x_copies[-1].start()

    next_x = 0
    for num, (first, end) in enumerate(gathers):
        send_y_rows(num, first, end)
        if first == 1:
            with jax.named_scope('pick_x'):
                build_pick(0, 1)
        if first == 0:
            for copy in (int_in, halo_in, w0_in, w1_in):
                copy.start()
        while next_x < len(x_parts) and x_parts[next_x][1] <= chunks[end - 1][1]:
            send_x_rows(next_x)
            next_x += 1

    with jax.named_scope('int_wait'):
        int_in.wait()
        halo_in.wait()
        w0_in.wait()
        w1_in.wait()
    with jax.named_scope('interior'):

        @pl.loop(0, nodes // BIG_COLS)
        def _(blk):
            cols = pl.ds(pl.multiple_of(blk * BIG_COLS, BIG_COLS), BIG_COLS)
            halo_t[:, cols] = halo_v[cols, :].T
            int_t[:, cols] = int_v[cols, :].T
            for lo, hi in big:
                z_int[lo:hi, cols] = dot(feat_v[lo:hi, :], int_v[cols, :], NT)

    def split3(value):
        high = value.astype(BF16)
        rest = value - high.astype(F32)
        middle = rest.astype(BF16)
        return high, middle, (rest - middle.astype(F32)).astype(BF16)

    last_lo, last_hi = chunks[-1]
    last = pl.ds(last_lo, last_hi - last_lo)
    tail = last_hi - last_lo
    with jax.named_scope('halo_pick'):
        halo_pick[...] = dot(halo_t[half:, :], pick_v[...], NN).astype(BF16)
    with jax.named_scope('xwait'):
        x_whole = remote(send_x, recv_v.at[:, :half], sx_sem, rx_sem, east)
        x_whole.wait_recv()
    with jax.named_scope('last_x'):
        z_last = z_int[last, :] + dot(recv_v[last, :half], halo_t[:half, :], NN)
        z_int[last, :] = z_last
        for num, piece in enumerate(split3(z_last)):
            z_split[num * LAST_ROWS:num * LAST_ROWS + tail, :] = piece
    with jax.named_scope('last_pick'):
        parts = dot(z_split[...], pick_v[...], NN)
        z_pick[...] = parts[:LAST_ROWS] + parts[LAST_ROWS:2 * LAST_ROWS] + parts[2 * LAST_ROWS:]

    groups = [(0, 3)] + [(num, num + 1) for num in range(3, len(chunks) - 1)]
    for first, end in groups:
        lo, hi = chunks[first][0], chunks[end - 1][1]
        with jax.named_scope(f'ywait{first}'):
            rows = pl.ds(lo, hi - lo)
            remote(send_y.at[rows, :], recv_v.at[rows, half:], sy_sem, ry_sem.at[max(first - 2, 0)], north).wait_recv()
        with jax.named_scope(f'yhalo{first}'):
            for col in range(0, nodes, HALO_COLS):
                cols = pl.ds(col, HALO_COLS)
                z_half[:hi - lo, cols] = (z_int[rows, cols] + dot(recv_v[rows, :], halo_t[:, cols], NN)).astype(BF16)
            part = dot(w0_ref[:, lo:hi], z_half[:hi - lo, :], NN)
            if first == 0:
                hid_acc[...] = part
            else:
                hid_acc[...] += part
    with jax.named_scope('hid_pick'):
        for num, piece in enumerate(split3(hid_acc[...])):
            hid_split[num * hid_rows:(num + 1) * hid_rows, :] = piece
        parts = dot(hid_split[...], pick_v[...], NN)
        hid_pick[...] = parts[:hid_rows] + parts[hid_rows:2 * hid_rows] + parts[2 * hid_rows:]

    second = [
        remote(send2_v.at[:, half:], recv2_v.at[:, half:], s2_sem, r2_sem.at[0], north),
        remote(send2_v.at[:, :quarter], recv2_v.at[:, :quarter], s2_sem, r2_sem.at[1], east),
        remote(send2_v.at[:, quarter:half], recv2_v.at[:, quarter:half], s2_sem, r2_sem.at[2], west),
    ]
    with jax.named_scope('ywait_last'):
        y_copies[-1].wait_recv()
    with jax.named_scope('sent2'):
        z_sent = (z_pick[:tail, :] + dot(recv_v[last, half:], halo_pick[...], NN)).astype(BF16)
        sent = hid_pick[...] + dot(w0_ref[:, last_lo:last_hi], z_sent, NN)
        send2_v[...] = jnp.maximum(sent, 0.0).astype(BF16)
    for copy in second:
        copy.start()
    with jax.named_scope('yhalo_last'):
        z_sum = (z_int[last, :] + dot(recv_v[last, half:], halo_t[half:, :], NN)).astype(BF16)
        hid_sum = hid_acc[...] + dot(w0_ref[:, last_lo:last_hi], z_sum, NN)
        hid_v[...] = jnp.maximum(hid_sum, 0.0).astype(BF16)
    with jax.named_scope('interior2'):
        hid_acc[...] = dot(hid_v[...], int_t[...], NN)
    from_y, from_west, from_east = second

    def halo_part(lo, hi):
        return dot(recv2_v[:, lo:hi], halo_t[lo:hi, :], NN)

    def finish(parts):
        z_sum = hid_acc[...]
        for num, (copies, lo, hi) in enumerate(parts):
            with jax.named_scope(f'finwait{num}'):
                for copy in copies:
                    copy.wait_recv()
            z_sum = z_sum + halo_part(lo, hi)
        out_ref[...] = dot(w1_ref[...], z_sum.astype(BF16), NN).astype(BF16)

    with jax.named_scope('halo2'):

        @pl.when(odd == 1)
        def _():
            finish([([from_y], half, slots), ([from_west], 0, quarter), ([from_east], quarter, half)])

        @pl.when(odd == 0)
        def _():
            finish([([from_east], quarter, half), ([from_west], 0, quarter), ([from_y], half, slots)])

    with jax.named_scope('sendwait'):
        for copy in (
            remote(send_y, recv_v.at[:, half:], sy_sem, ry_sem.at[0], north),
            x_whole,
            remote(send2_v, recv2_v, s2_sem, r2_sem.at[0], north),
        ):
            copy.wait_send()


def solution(mesh):
    grid_y = mesh.shape['tiley']
    grid_x = mesh.shape['tilex']
    node_spec = P(('parts', 'tiley', 'tilex'), None)
    full_spec = P(None, None)

    def per_device(node_feats, adj_int, adj_halo, send_idx, w_hidden, w_out):
        nodes, feat = node_feats.shape
        slots = adj_halo.shape[1]
        half, quarter = slots // 2, slots // 4
        hidden, classes = w_out.shape
        chunks = feature_chunks(feat)
        x_parts = x_chunks(feat)
        big = big_chunks(feat)
        vmem = pl.BlockSpec(memory_space=pltpu.VMEM)
        hbm = pl.BlockSpec(memory_space=pl.ANY)
        dma = pltpu.SemaphoreType.DMA
        out = pl.pallas_call(
            functools.partial(gcn_kernel, grid_y, grid_x, chunks, x_parts, big),
            out_shape=pltpu.VMEM((classes, nodes), BF16),
            in_specs=[hbm] * 6,
            out_specs=vmem,
            scratch_shapes=[
                pltpu.VMEM(send_idx.shape, jnp.int32),
                pltpu.VMEM((hidden, feat), BF16),
                pltpu.VMEM((classes, hidden), BF16),
                pltpu.VMEM((feat, nodes), BF16),
                pltpu.VMEM((nodes, nodes), BF16),
                pltpu.VMEM((nodes, nodes), BF16),
                pltpu.VMEM((nodes, slots), BF16),
                pltpu.VMEM((slots, nodes), BF16),
                pltpu.VMEM((nodes, slots), BF16),
                pltpu.VMEM((feat, half), BF16),
                pltpu.VMEM((feat, half), BF16),
                pltpu.VMEM((feat, slots), BF16),
                pltpu.VMEM((feat, nodes), F32),
                pltpu.VMEM((512, nodes), BF16),
                pltpu.VMEM((half, slots), BF16),
                pltpu.VMEM((3 * LAST_ROWS, nodes), BF16),
                pltpu.VMEM((LAST_ROWS, slots), F32),
                pltpu.VMEM((3 * hidden, nodes), BF16),
                pltpu.VMEM((hidden, slots), F32),
                pltpu.VMEM((hidden, nodes), F32),
                pltpu.VMEM((hidden, nodes), BF16),
                pltpu.VMEM((hidden, slots), BF16),
                pltpu.VMEM((hidden, slots), BF16),
                dma((3,)),
                dma((NUM_GATHERS,)),
                dma,
                dma,
                dma,
                dma((len(chunks) - 2,)),
                dma,
                dma,
                dma,
                dma((3,)),
                pltpu.SemaphoreType.REGULAR,
            ],
            compiler_params=pltpu.CompilerParams(collective_id=0, has_side_effects=True, vmem_limit_bytes=60 * 2**20),
        )(send_idx, w_hidden.T, w_out.T, node_feats.T, adj_int, adj_halo)
        return out.T

    return jax.shard_map(per_device, mesh=mesh, in_specs=(node_spec, node_spec, node_spec, node_spec, full_spec, full_spec), out_specs=node_spec, check_vma=False)
```

```python
import functools

import jax
import jax.numpy as jnp
from jax import lax
from jax.experimental import pallas as pl
from jax.experimental.pallas import tpu as pltpu
from jax.sharding import PartitionSpec as P

BF16 = jnp.bfloat16
F32 = jnp.float32
MESH = pl.DeviceIdType.MESH
N_TILE = 256
BIG_ROWS = 512
LAST_ROWS = 112
NUM_GATHERS = 3
BIG_COLS = 2048
HALO_COLS = 512
NN = (((1,), (0,)), ((), ()))
NT = (((1,), (1,)), ((), ()))


def dot(lhs, rhs, dims):
    return lax.dot_general(lhs, rhs, dims, preferred_element_type=F32)


def feature_chunks(feat):
    last = (feat - 96) // 16 * 16
    cuts = [0, 64, 256]
    while last - 128 - cuts[-1] > 256:
        cuts.append(cuts[-1] + 256)
    cuts += [last - 128, last, feat]
    return list(zip(cuts[:-1], cuts[1:]))


def big_chunks(feat):
    return [(lo, min(lo + BIG_ROWS, feat)) for lo in range(0, feat, BIG_ROWS)]


def x_chunks(feat):
    return [(0, BIG_ROWS), (BIG_ROWS, feat)]


def gcn_kernel(grid_y, grid_x, chunks, x_parts, big, idx_hbm, w0_hbm, w1_hbm, feat_hbm, int_hbm, halo_hbm, out_ref,
               idx_ref, w0_ref, w1_ref, feat_v, int_v, int_t, halo_v, halo_t, pick_v, send_y, send_x, recv_v, z_int, z_half, halo_pick, z_split, z_pick, hid_split, hid_pick, hid_acc,
               hid_v, send2_v, recv2_v,
               small_sem, feat_sem, int_sem, halo_sem, sy_sem, ry_sem, sx_sem, rx_sem, s2_sem, r2_sem, even_sem):
    me_y = lax.axis_index('tiley')
    me_x = lax.axis_index('tilex')
    east = {'tilex': lax.rem(me_x + 1, grid_x)}
    west = {'tilex': lax.rem(me_x + grid_x - 1, grid_x)}
    north = {'tiley': lax.rem(me_y + 1, grid_y)}
    nodes = int_v.shape[0]
    slots = halo_v.shape[1]
    half = slots // 2
    quarter = half // 2
    hid_rows = hid_v.shape[0]

    barrier = pltpu.get_barrier_semaphore()
    pl.semaphore_signal(barrier, inc=1, device_id=north, device_id_type=MESH)
    odd = lax.rem(me_x, 2)

    @pl.when(odd == 1)
    def _():
        for neighbour in (east, west):
            pl.semaphore_signal(barrier, inc=1, device_id=neighbour, device_id_type=MESH)

    idx_in = pltpu.make_async_copy(idx_hbm, idx_ref, small_sem.at[0])
    gathers = [(0, 1), (1, 2), (2, 4), (4, len(chunks))]
    feat_in = []
    for num, (first, end) in enumerate(gathers[:2] + [(2, len(chunks))]):
        rows = pl.ds(chunks[first][0], chunks[end - 1][1] - chunks[first][0])
        feat_in.append(pltpu.make_async_copy(feat_hbm.at[rows, :], feat_v.at[rows, :], feat_sem.at[num]))
    w0_in = pltpu.make_async_copy(w0_hbm, w0_ref, small_sem.at[1])
    w1_in = pltpu.make_async_copy(w1_hbm, w1_ref, small_sem.at[2])
    int_in = pltpu.make_async_copy(int_hbm, int_v, int_sem)
    halo_in = pltpu.make_async_copy(halo_hbm, halo_v, halo_sem)
    idx_in.start()
    feat_in[0].start()

    def pick_block(buf, start):
        node_ids = lax.broadcasted_iota(jnp.int16, (N_TILE, quarter), 0)
        plan = jnp.broadcast_to(idx_ref[buf:buf + 1, :] - start, (N_TILE, quarter)).astype(jnp.int16)
        return jnp.where(node_ids == plan, jnp.ones((), BF16), jnp.zeros((), BF16))

    def build_pick(*bufs):
        @pl.loop(0, nodes // N_TILE)
        def _(blk):
            start = pl.multiple_of(blk * N_TILE, N_TILE)
            for buf in bufs:
                pick_v[pl.ds(start, N_TILE), buf * quarter:(buf + 1) * quarter] = pick_block(buf, start)

    def remote(src, dst, send_sem, recv_sem, target):
        return pltpu.make_async_remote_copy(src_ref=src, dst_ref=dst, send_sem=send_sem, recv_sem=recv_sem, device_id=target, device_id_type=MESH)

    with jax.named_scope('idx_wait'):
        idx_in.wait()
    for copy in feat_in[1:]:
        copy.start()
    y_copies = []
    x_copies = []

    def first_piece(rows):
        picked = None
        for start in range(0, nodes, N_TILE):
            block = jnp.concatenate([pick_block(2, start), pick_block(3, start)], axis=1)
            pick_v[start:start + N_TILE, half:] = block
            part = dot(feat_v[rows, start:start + N_TILE], block, NN)
            picked = part if picked is None else picked + part
        send_y[rows, :] = picked.astype(BF16)

    def send_y_rows(num, first, end):
        lo, hi = chunks[first][0], chunks[end - 1][1]
        rows = pl.ds(lo, hi - lo)
        with jax.named_scope(f'feat_wait{first}'):
            if num < len(feat_in):
                feat_in[num].wait()
        with jax.named_scope(f'gather_y{first}'):
            if first > 0:
                send_y[rows, :] = dot(feat_v[rows, :], pick_v[:, half:], NN).astype(BF16)
            else:
                first_piece(rows)
        if first == 0:
            with jax.named_scope('barrier'):
                pl.semaphore_wait(barrier, 3 - 2 * odd)

                @pl.when(odd == 0)
                def _():
                    for neighbour in (east, west):
                        pl.semaphore_signal(even_sem, inc=1, device_id=neighbour, device_id_type=MESH)

        for chunk in range(first, end):
            rows = pl.ds(chunks[chunk][0], chunks[chunk][1] - chunks[chunk][0])
            y_copies.append(remote(send_y.at[rows, :], recv_v.at[rows, half:], sy_sem, ry_sem.at[max(chunk - 2, 0)], north))
            y_copies[-1].start()

    def send_x_rows(num):
        rows = pl.ds(x_parts[num][0], x_parts[num][1] - x_parts[num][0])
        with jax.named_scope(f'gather_x{num}'):
            picked = dot(feat_v[rows, :], pick_v[:, :half], NN).astype(BF16)
            send_x[rows, :] = picked
        if num == 0:

            @pl.when(odd == 1)
            def _():
                pl.semaphore_wait(even_sem, 2)

        x_copies.append(remote(send_x.at[rows, :quarter], recv_v.at[rows, :quarter], sx_sem, rx_sem, east))
        x_copies.append(remote(send_x.at[rows, quarter:], recv_v.at[rows, quarter:half], sx_sem, rx_sem, west))
        x_copies[-2].start()
        x_copies[-1].start()

    next_x = 0
    for num, (first, end) in enumerate(gathers):
        send_y_rows(num, first, end)
        if first == 1:
            with jax.named_scope('pick_x'):
                build_pick(0, 1)
        if first == 0:
            for copy in (int_in, halo_in, w0_in, w1_in):
                copy.start()
        while next_x < len(x_parts) and x_parts[next_x][1] <= chunks[end - 1][1]:
            send_x_rows(next_x)
            next_x += 1

    with jax.named_scope('int_wait'):
        int_in.wait()
        halo_in.wait()
        w0_in.wait()
        w1_in.wait()
    with jax.named_scope('interior'):

        @pl.loop(0, nodes // BIG_COLS)
        def _(blk):
            cols = pl.ds(pl.multiple_of(blk * BIG_COLS, BIG_COLS), BIG_COLS)
            halo_t[:, cols] = halo_v[cols, :].T
            int_t[:, cols] = int_v[cols, :].T
            for lo, hi in big:
                z_int[lo:hi, cols] = dot(feat_v[lo:hi, :], int_v[cols, :], NT)

    def split3(value):
        high = value.astype(BF16)
        rest = value - high.astype(F32)
        middle = rest.astype(BF16)
        return high, middle, (rest - middle.astype(F32)).astype(BF16)

    last_lo, last_hi = chunks[-1]
    last = pl.ds(last_lo, last_hi - last_lo)
    tail = last_hi - last_lo
    with jax.named_scope('halo_pick'):
        halo_pick[...] = dot(halo_t[half:, :], pick_v[...], NN).astype(BF16)
    with jax.named_scope('xwait'):
        x_whole = remote(send_x, recv_v.at[:, :half], sx_sem, rx_sem, east)
        x_whole.wait_recv()
    with jax.named_scope('last_x'):
        z_last = z_int[last, :] + dot(recv_v[last, :half], halo_t[:half, :], NN)
        z_int[last, :] = z_last
        for num, piece in enumerate(split3(z_last)):
            z_split[num * LAST_ROWS:num * LAST_ROWS + tail, :] = piece
    with jax.named_scope('last_pick'):
        parts = dot(z_split[...], pick_v[...], NN)
        z_pick[...] = parts[:LAST_ROWS] + parts[LAST_ROWS:2 * LAST_ROWS] + parts[2 * LAST_ROWS:]

    groups = [(0, 3)] + [(num, num + 1) for num in range(3, len(chunks) - 1)]
    for first, end in groups:
        lo, hi = chunks[first][0], chunks[end - 1][1]
        with jax.named_scope(f'ywait{first}'):
            rows = pl.ds(lo, hi - lo)
            remote(send_y.at[rows, :], recv_v.at[rows, half:], sy_sem, ry_sem.at[max(first - 2, 0)], north).wait_recv()
        with jax.named_scope(f'yhalo{first}'):
            for col in range(0, nodes, HALO_COLS):
                cols = pl.ds(col, HALO_COLS)
                z_half[:hi - lo, cols] = (z_int[rows, cols] + dot(recv_v[rows, :], halo_t[:, cols], NN)).astype(BF16)
            part = dot(w0_ref[:, lo:hi], z_half[:hi - lo, :], NN)
            if first == 0:
                hid_acc[...] = part
            else:
                hid_acc[...] += part
    with jax.named_scope('hid_pick'):
        for num, piece in enumerate(split3(hid_acc[...])):
            hid_split[num * hid_rows:(num + 1) * hid_rows, :] = piece
        parts = dot(hid_split[...], pick_v[...], NN)
        hid_pick[...] = parts[:hid_rows] + parts[hid_rows:2 * hid_rows] + parts[2 * hid_rows:]

    second = [
        remote(send2_v.at[:, half:], recv2_v.at[:, half:], s2_sem, r2_sem.at[0], north),
        remote(send2_v.at[:, :quarter], recv2_v.at[:, :quarter], s2_sem, r2_sem.at[1], east),
        remote(send2_v.at[:, quarter:half], recv2_v.at[:, quarter:half], s2_sem, r2_sem.at[2], west),
    ]
    with jax.named_scope('ywait_last'):
        y_copies[-1].wait_recv()
    with jax.named_scope('sent2'):
        z_sent = (z_pick[:tail, :] + dot(recv_v[last, half:], halo_pick[...], NN)).astype(BF16)
        sent = hid_pick[...] + dot(w0_ref[:, last_lo:last_hi], z_sent, NN)
        send2_v[...] = jnp.maximum(sent, 0.0).astype(BF16)
    for copy in second:
        copy.start()
    with jax.named_scope('yhalo_last'):
        z_sum = (z_int[last, :] + dot(recv_v[last, half:], halo_t[half:, :], NN)).astype(BF16)
        hid_sum = hid_acc[...] + dot(w0_ref[:, last_lo:last_hi], z_sum, NN)
        hid_v[...] = jnp.maximum(hid_sum, 0.0).astype(BF16)
    with jax.named_scope('interior2'):
        hid_acc[...] = dot(hid_v[...], int_t[...], NN)
    from_y, from_west, from_east = second

    def halo_part(lo, hi):
        return dot(recv2_v[:, lo:hi], halo_t[lo:hi, :], NN)

    def finish(parts):
        z_sum = hid_acc[...]
        for num, (copies, lo, hi) in enumerate(parts):
            with jax.named_scope(f'finwait{num}'):
                for copy in copies:
                    copy.wait_recv()
            z_sum = z_sum + halo_part(lo, hi)
        out_ref[...] = dot(w1_ref[...], z_sum.astype(BF16), NN).astype(BF16)

    with jax.named_scope('halo2'):

        @pl.when(odd == 1)
        def _():
            finish([([from_y], half, slots), ([from_west], 0, quarter), ([from_east], quarter, half)])

        @pl.when(odd == 0)
        def _():
            finish([([from_east], quarter, half), ([from_west], 0, quarter), ([from_y], half, slots)])

    with jax.named_scope('sendwait'):
        for copy in (
            remote(send_y, recv_v.at[:, half:], sy_sem, ry_sem.at[0], north),
            x_whole,
            remote(send2_v, recv2_v, s2_sem, r2_sem.at[0], north),
        ):
            copy.wait_send()


def solution(mesh):
    grid_y = mesh.shape['tiley']
    grid_x = mesh.shape['tilex']
    node_spec = P(('parts', 'tiley', 'tilex'), None)
    full_spec = P(None, None)

    def per_device(node_feats, adj_int, adj_halo, send_idx, w_hidden, w_out):
        nodes, feat = node_feats.shape
        slots = adj_halo.shape[1]
        half, quarter = slots // 2, slots // 4
        hidden, classes = w_out.shape
        chunks = feature_chunks(feat)
        x_parts = x_chunks(feat)
        big = big_chunks(feat)
        vmem = pl.BlockSpec(memory_space=pltpu.VMEM)
        hbm = pl.BlockSpec(memory_space=pl.ANY)
        dma = pltpu.SemaphoreType.DMA
        out = pl.pallas_call(
            functools.partial(gcn_kernel, grid_y, grid_x, chunks, x_parts, big),
            out_shape=pltpu.VMEM((classes, nodes), BF16),
            in_specs=[hbm] * 6,
            out_specs=vmem,
            scratch_shapes=[
                pltpu.VMEM(send_idx.shape, jnp.int32),
                pltpu.VMEM((hidden, feat), BF16),
                pltpu.VMEM((classes, hidden), BF16),
                pltpu.VMEM((feat, nodes), BF16),
                pltpu.VMEM((nodes, nodes), BF16),
                pltpu.VMEM((nodes, nodes), BF16),
                pltpu.VMEM((nodes, slots), BF16),
                pltpu.VMEM((slots, nodes), BF16),
                pltpu.VMEM((nodes, slots), BF16),
                pltpu.VMEM((feat, half), BF16),
                pltpu.VMEM((feat, half), BF16),
                pltpu.VMEM((feat, slots), BF16),
                pltpu.VMEM((feat, nodes), F32),
                pltpu.VMEM((512, nodes), BF16),
                pltpu.VMEM((half, slots), BF16),
                pltpu.VMEM((3 * LAST_ROWS, nodes), BF16),
                pltpu.VMEM((LAST_ROWS, slots), F32),
                pltpu.VMEM((3 * hidden, nodes), BF16),
                pltpu.VMEM((hidden, slots), F32),
                pltpu.VMEM((hidden, nodes), F32),
                pltpu.VMEM((hidden, nodes), BF16),
                pltpu.VMEM((hidden, slots), BF16),
                pltpu.VMEM((hidden, slots), BF16),
                dma((3,)),
                dma((NUM_GATHERS,)),
                dma,
                dma,
                dma,
                dma((len(chunks) - 2,)),
                dma,
                dma,
                dma,
                dma((3,)),
                pltpu.SemaphoreType.REGULAR,
            ],
            compiler_params=pltpu.CompilerParams(collective_id=0, has_side_effects=True, vmem_limit_bytes=60 * 2**20),
        )(send_idx, w_hidden.T, w_out.T, node_feats.T, adj_int, adj_halo)
        return out.T

    return jax.shard_map(per_device, mesh=mesh, in_specs=(node_spec, node_spec, node_spec, node_spec, full_spec, full_spec), out_specs=node_spec, check_vma=False)
```
